512 devices in a mesh: row: 32 (over z_hi, x, core), col: 16 (over y, z_lo).
Axes of the slice: x: 4, y: 8, z: 8 (z_hi: 4, z_lo: 2; z = z_hi * 2 + z_lo), core: 2. Of those that a mesh axis runs over, the one named last changes fastest.
Arguments:
- kernel: bfloat16 [20480, 20480], P('row', 'col'), as said below
- labels: int32 [20480], P('row'), may hold values from -1 to 1, as said below
- start_dual: float32 [20480, 128], P('row'), may hold values from 0 to 1
- penalty: float32 [128], replicated, may hold values from 2 to 6
- box: float32 [128], replicated, may hold values from 0.1 to 1
Outputs:
- dual: float32 [20480, 128], P(('row', 'col'))
- scaled_mult: float32 [20480, 128], P(('row', 'col'))
- gaps: float32 [3, 128], replicated
- offset: float32 [128], replicated
The draws below stay inside these ranges and needn't reach their ends.
Inputs may be any that keep to these rules, and one draw needn't show every extreme that they name: `labels`: each entry is -1 or +1. `kernel`: a symmetric matrix.
All inputs are finite; a program needn't handle non-finite values.
Results may differ from the reference program's by a relative error of at most 0.0027.
Values may be sent and summed in bfloat16 or wider, within the bound.
A program may use at most 64 MiB of HBM per device.

```python
import math
import jax
import jax.numpy as jnp

SETTINGS = 128
ITERS = 3
EXAMPLES = 20480


def draw_kernel(key, part):
    noise = jax.random.normal(key, (EXAMPLES, EXAMPLES), jnp.float32)
    sym = (noise + noise.T) * 0.5
    result = jnp.eye(EXAMPLES, dtype=jnp.float32) + sym * (0.7 / jnp.sqrt(2.0 * EXAMPLES))
    return result.astype(jnp.bfloat16)


def draw_labels(key, part):
    return 2 * jax.random.randint(key, (EXAMPLES,), 0, 2, dtype=jnp.int32) - 1


def shard_levels(key, dims, split, least, high):
    factor_of = 1.0
    for dim, shards_of in split:
        draws = jax.random.uniform(jax.random.fold_in(jax.random.fold_in(key, 6), dim), (shards_of,), jnp.float32, least / len(split), high / len(split))
        factor_of = factor_of * jnp.repeat(jnp.exp(draws), dims[dim] // shards_of).reshape((-1,) + (1,) * (len(dims) - 1 - dim))
    return factor_of


def setup_inputs(seed: int = 0) -> dict:
    streams_of = jax.random.split(jax.random.key(seed), 6)
    return {
        "kernel": draw_kernel(jax.random.fold_in(streams_of[5], 71), 0),
        "labels": draw_labels(jax.random.fold_in(streams_of[5], 71), 0),
        "start_dual": jnp.clip(1.0 * jax.random.uniform(streams_of[2], (EXAMPLES, SETTINGS), jnp.float32) ** shard_levels(streams_of[2], (EXAMPLES, SETTINGS), ((0, 32),), -0.2, 0.2), 0.0, 1.0),
        "penalty": jnp.clip(jnp.exp(jax.random.uniform(streams_of[3], (SETTINGS,), jnp.float32, math.log(2.0), math.log(6.0))), 2.0, 6.0),
        "box": jnp.clip(jnp.exp(jax.random.uniform(streams_of[4], (SETTINGS,), jnp.float32, math.log(0.1), math.log(1.0))), 0.1, 1.0),
    }


def reference(kernel, labels, start_dual, penalty, box):
    total = kernel.shape[0]
    signs = labels.astype(jnp.float32)[:, None]
    dual = jnp.minimum(jnp.maximum(start_dual, 0.0), box[None, :])
    scaled_mult = jnp.zeros_like(dual)
    gap_list = []
    offset = jnp.zeros(box.shape, jnp.float32)
    for step in range(ITERS):
        products = (signs * dual).astype(jnp.bfloat16)
        q_value = signs * jnp.dot(kernel, products, preferred_element_type=jnp.float32)
        w_value = dual - scaled_mult - (q_value - 1.0) / penalty[None, :]
        offset = jnp.sum(signs * w_value, axis=0) / total
        hinge = jnp.maximum(0.0, 1.0 - q_value - signs * offset[None, :])
        gap_terms = dual * q_value - dual + box[None, :] * hinge
        gap_list.append(jnp.sum(gap_terms, axis=0) / total)
        x_value = w_value - signs * offset[None, :]
        dual = jnp.minimum(jnp.maximum(x_value + scaled_mult, 0.0), box[None, :])
        scaled_mult = scaled_mult + x_value - dual
    return dual, scaled_mult, jnp.stack(gap_list), offset
```

```python
import functools

import jax
import jax.numpy as jnp
from jax import lax
from jax.experimental import pallas as pl
from jax.experimental.pallas import tpu as pltpu
from jax.sharding import Mesh
from jax.sharding import PartitionSpec as P

ITERS = 3
ROW = ("row_0", "row_1", "row_2")
COL = ("col_0", "col_1")
ROW_COL = ROW + COL
MESH = pl.DeviceIdType.MESH
F32 = jnp.float32
BF16 = jnp.bfloat16


def loop(low, high, step):
    def one(i, carry):
        step(i)
        return carry

    lax.fori_loop(low, high, one, jnp.int32(0))


def remote(src, dst, send, recv, device):
    return pltpu.make_async_remote_copy(
        src_ref=src, dst_ref=dst, send_sem=send, recv_sem=recv, device_id=device, device_id_type=MESH
    )


def admm(
    dims, total,
    kernel_hbm, labels_hbm, start_hbm, penalty_ref, box_ref,
    dual_out, mult_out, gaps_out, offset_out,
    kernel_ref, labels_ref, start_ref, signs_ref, part_ref, load_sem,
    state_send, state_recv, state_ss, state_rs,
    core_send, core_recv, core_ss, core_rs,
    row_send, row_recv, row_ss, row_rs,
    gat_ref, gat_ss, gat_rs, fwd_ss,
    col_send, col_recv, col_ss, col_rs,
    pcol_ref, pcol_ss, pcol_rs,
    near_ref, near_ss, near_rs,
    far_ref, far_ss, far_rs,
):
    hs, xs, ks, ys, ls = dims
    groups, rows, cols = hs * xs, hs * xs * ks, ys * ls
    h, x, k = (lax.axis_index(a) for a in ROW)
    y, l = (lax.axis_index(a) for a in COL)
    g = h * xs + x
    r = g * ks + k
    c = y * ls + l
    piece = state_send.shape[2]
    near_n, far_n = ys * ks, hs * xs * ls
    near_me = y * ks + k
    far_me = g * ls + l
    other = 1 - k

    def chip(to):
        return {"row_0": lax.div(to, xs), "row_1": lax.rem(to, xs)}

    def column(to):
        return {"col_0": lax.div(to, ls), "col_1": lax.rem(to, ls)}

    def whole(row, col):
        return {
            "row_0": lax.div(row, xs * ks), "row_1": lax.rem(lax.div(row, ks), xs), "row_2": lax.rem(row, ks),
            "col_0": lax.div(col, ls), "col_1": lax.rem(col, ls),
        }

    def near(to):
        return {"col_0": lax.div(to, ks), "row_2": lax.rem(to, ks)}

    def far(to):
        return {
            "row_0": lax.div(to, xs * ls), "row_1": lax.rem(lax.div(to, ls), xs), "col_1": lax.rem(to, ls)
        }

    partner = {"row_2": other}
    mine = g * ks + other
    block = r * cols + c
    to_piece = lax.rem(block, rows)
    to_column = whole(
        lax.div(to_piece, ks) * ks + (ks - 1 - lax.rem(to_piece, ks)), lax.div(block, rows)
    )
    owned = c * rows + mine
    to_row = whole(lax.div(owned, cols), lax.rem(owned, cols))

    load_k = pltpu.make_async_copy(kernel_hbm, kernel_ref, load_sem.at[0])
    load_s = pltpu.make_async_copy(start_hbm, start_ref, load_sem.at[1])
    load_l = pltpu.make_async_copy(labels_hbm, labels_ref, load_sem.at[2])
    load_l.start()
    load_s.start()
    load_k.start()

    barrier = pltpu.get_barrier_semaphore()

    def greet(device):
        pl.semaphore_signal(barrier, inc=1, device_id=device, device_id_type=MESH)

    greet(to_column)
    greet(to_row)
    loop(1, far_n, lambda i: greet(far(lax.rem(far_me + i, far_n))))
    loop(1, near_n, lambda i: greet(near(lax.rem(near_me + i, near_n))))
    crossed = ys * (ls - 1)
    if crossed:
        def cross(i):
            greet({"col_0": lax.rem(i, ys), "col_1": lax.rem(l + 1 + lax.div(i, ys), ls)})
        loop(0, crossed, cross)

    penalty = penalty_ref[...]
    box = box_ref[...]
    load_l.wait()
    load_s.wait()
    wide = labels_ref.shape[1]
    for i in range(labels_ref.shape[0]):
        line = labels_ref[i : i + 1, :].astype(F32)
        if wide == 128:
            block_signs = jnp.transpose(jnp.broadcast_to(line, (128, 128)))
        else:
            block_signs = jnp.broadcast_to(jnp.transpose(line), (wide, 128))
        signs_ref[i * wide : (i + 1) * wide, :] = block_signs
    first = jnp.minimum(jnp.maximum(start_ref[...], 0.0), box)
    start_ref[...] = first
    weighted = (signs_ref[...] * first).astype(BF16)
    own_rows = pl.ds(pl.multiple_of(c * piece, 8), piece)
    signs_row = signs_ref[own_rows, :]
    dual = start_ref[own_rows, :]
    mult = jnp.zeros_like(dual)
    state_send[0, 0] = dual
    state_send[0, 1] = signs_row

    def move_state(t, device):
        remote(state_send.at[t], state_recv.at[t], state_ss.at[t], state_rs.at[t], device).start()

    def arrived_state(t):
        remote(state_send.at[t], state_recv.at[t], state_ss.at[t], state_rs.at[t], to_row).wait_recv()
        return state_recv[t, 0], state_recv[t, 1]

    def near_copy(t, i):
        return remote(near_ref.at[t, near_me], near_ref.at[t, near_me], near_ss.at[t, i], near_rs.at[t, near_me], near(i))

    def near_wait(t, i):
        return remote(near_ref.at[t, i], near_ref.at[t, i], near_ss.at[t, i], near_rs.at[t, i], near(i))

    def far_copy(t, i):
        return remote(far_ref.at[t, far_me], far_ref.at[t, far_me], far_ss.at[t, i], far_rs.at[t, far_me], far(i))

    def far_wait(t, i):
        return remote(far_ref.at[t, i], far_ref.at[t, i], far_ss.at[t, i], far_rs.at[t, i], far(i))

    def sum_start(t, top, bottom):
        near_ref[t, near_me, 0:1, :] = top
        near_ref[t, near_me, 1:2, :] = bottom
        loop(1, near_n, lambda i: near_copy(t, lax.rem(near_me + i, near_n)).start())

    def sum_middle(t):
        loop(1, near_n, lambda i: near_wait(t, lax.rem(near_me + i, near_n)).wait_recv())
        far_ref[t, far_me] = jnp.sum(near_ref[t], axis=0)
        loop(1, far_n, lambda i: far_copy(t, lax.rem(far_me + i, far_n)).start())

    def sum_end(t):
        loop(1, far_n, lambda i: far_wait(t, lax.rem(far_me + i, far_n)).wait_recv())
        return jnp.sum(far_ref[t], axis=0)

    def local_bias(dual, mult, signs, product_sum):
        steady = jnp.sum(signs * (dual - mult), axis=0, keepdims=True)
        return steady - (product_sum - jnp.sum(signs, axis=0, keepdims=True)) / penalty

    def update(q, dual, mult, signs, offset):
        w = dual - mult - (q - 1.0) / penalty
        hinge = jnp.maximum(0.0, 1.0 - q - signs * offset)
        gap = jnp.sum(dual * q - dual + box * hinge, axis=0, keepdims=True)
        x_value = w - signs * offset
        dual_next = jnp.minimum(jnp.maximum(x_value + mult, 0.0), box)
        return dual_next, mult + x_value - dual_next, gap

    def row_copy(s, i):
        return remote(row_send.at[s, i], row_recv.at[s, g], row_ss.at[s, i], row_rs.at[s, g], chip(i))

    def row_wait(s, i):
        return remote(row_send.at[s, i], row_recv.at[s, i], row_ss.at[s, i], row_rs.at[s, i], chip(i))

    def core_copy(s):
        return remote(core_send.at[s], core_recv.at[s], core_ss.at[s], core_rs.at[s], partner)

    def transposed_start(s, weighted):
        product = lax.dot_general(
            kernel_ref[...], weighted, (((0,), (0,)), ((), ())), preferred_element_type=F32
        )
        part_ref[...] = product.reshape(part_ref.shape)
        core_send[s] = part_ref[:, k].astype(BF16)
        return jnp.sum(product, axis=0, keepdims=True)

    def transposed_send(s):
        core_copy(s).wait_recv()
        both = part_ref[:, other] + core_recv[s].astype(F32)
        part_ref[:, other] = both
        row_send[s] = both.astype(BF16)
        loop(1, groups, lambda i: row_copy(s, lax.rem(g + i, groups)).start())

    def transposed_sum(s):
        row_recv[s, g] = jnp.zeros(row_recv.shape[2:], BF16)
        loop(1, groups, lambda i: row_wait(s, lax.rem(g + i, groups)).wait_recv())
        return part_ref[g, other] + jnp.sum(row_recv[s].astype(F32), axis=0)

    zero = jnp.zeros((1, box.shape[1]), F32)

    load_k.wait()
    product_sum = transposed_start(0, weighted)
    pl.semaphore_wait(barrier, 2 + far_n - 1 + near_n - 1 + crossed)
    core_copy(0).start()
    sum_start(0, local_bias(dual, mult, signs_row, product_sum), zero)
    move_state(0, to_column)
    transposed_send(0)
    sum_middle(0)
    q_sum = transposed_sum(0)
    dual, signs_col = arrived_state(0)
    mult = jnp.zeros_like(dual)
    offset = sum_end(0)[0:1] / total
    dual, mult, gap = update(signs_col * q_sum, dual, mult, signs_col, offset)

    gat_ref[mine] = (signs_col * dual).astype(BF16)

    def gat_copy(slot, send, device):
        return remote(gat_ref.at[slot], gat_ref.at[slot], send, gat_rs.at[slot], device)

    loop(1, groups, lambda i: gat_copy(mine, gat_ss.at[lax.rem(g + i, groups)], chip(lax.rem(g + i, groups))).start())
    gat_copy(mine, fwd_ss.at[g], partner).start()
    state_send[1, 0] = dual
    state_send[1, 1] = mult
    move_state(1, to_row)

    def forward(i):
        to = lax.rem(g + i, groups)
        slot = to * ks + other
        gat_copy(slot, fwd_ss.at[to], partner).wait_recv()
        gat_copy(slot, fwd_ss.at[to], partner).start()

    loop(1, groups, forward)
    loop(0, groups, lambda i: gat_copy(i * ks + k, fwd_ss.at[i], partner).wait_recv())
    gathered = gat_ref[...].astype(F32).reshape(rows * piece, -1).astype(BF16)
    product = jnp.dot(kernel_ref[...], gathered, preferred_element_type=F32)
    col_send[...] = product.reshape(col_send.shape).astype(BF16)
    part_ref[0 : cols // ks] = product.reshape(cols // ks, ks, piece, -1)

    def col_copy(i):
        return remote(col_send.at[i], col_recv.at[c], col_ss.at[i], col_rs.at[c], column(i))

    def col_wait(i):
        return remote(col_send.at[i], col_recv.at[i], col_ss.at[i], col_rs.at[i], column(i))

    sum_start(1, local_bias(dual, mult, signs_col, jnp.sum(product, axis=0, keepdims=True)), gap)
    loop(1, cols, lambda i: col_copy(lax.rem(c + i, cols)).start())
    sum_middle(1)
    col_recv[c] = jnp.zeros(col_recv.shape[1:], BF16)
    loop(1, cols, lambda i: col_wait(lax.rem(c + i, cols)).wait_recv())
    q_sum = part_ref[lax.div(c, ks), lax.rem(c, ks)] + jnp.sum(col_recv[...].astype(F32), axis=0)
    dual, mult = arrived_state(1)
    sums = sum_end(1)
    gaps_out[0:1, :] = sums[1:2] / total
    offset = sums[0:1] / total
    dual, mult, gap = update(signs_row * q_sum, dual, mult, signs_row, offset)

    pcol_ref[c] = (signs_row * dual).astype(BF16)

    def pcol_copy(i):
        return remote(pcol_ref.at[c], pcol_ref.at[c], pcol_ss.at[i], pcol_rs.at[c], column(i))

    def pcol_wait(i):
        return remote(pcol_ref.at[i], pcol_ref.at[i], pcol_ss.at[i], pcol_rs.at[i], column(i))

    loop(1, cols, lambda i: pcol_copy(lax.rem(c + i, cols)).start())
    state_send[2, 0] = dual
    state_send[2, 1] = mult
    move_state(2, to_column)
    loop(1, cols, lambda i: pcol_wait(lax.rem(c + i, cols)).wait_recv())
    weighted = pcol_ref[...].astype(F32).reshape(cols * piece, -1).astype(BF16)
    product_sum = transposed_start(1, weighted)
    core_copy(1).start()
    sum_start(2, local_bias(dual, mult, signs_row, product_sum), gap)
    transposed_send(1)
    sum_middle(2)
    q_sum = transposed_sum(1)
    dual, mult = arrived_state(2)
    sums = sum_end(2)
    gaps_out[1:2, :] = sums[1:2] / total
    offset = sums[0:1] / total
    dual, mult, gap = update(signs_col * q_sum, dual, mult, signs_col, offset)

    sum_start(3, zero, gap)
    state_send[3, 0] = dual
    state_send[3, 1] = mult
    move_state(3, to_row)
    offset_out[...] = offset
    sum_middle(3)
    dual, mult = arrived_state(3)
    dual_out[...] = dual
    mult_out[...] = mult
    gaps_out[2:3, :] = sum_end(3)[1:2] / total

    for t in range(4):
        remote(state_send.at[t], state_recv.at[t], state_ss.at[t], state_rs.at[t], to_row).wait_send()
        loop(1, near_n, lambda i: near_wait(t, lax.rem(near_me + i, near_n)).wait_send())
        loop(1, far_n, lambda i: far_wait(t, lax.rem(far_me + i, far_n)).wait_send())
    for s in range(2):
        core_copy(s).wait_send()
        loop(1, groups, lambda i: row_wait(s, lax.rem(g + i, groups)).wait_send())
    loop(1, groups, lambda i: gat_copy(mine, gat_ss.at[lax.rem(g + i, groups)], partner).wait_send())
    loop(0, groups, lambda i: gat_copy(i * ks + other, fwd_ss.at[i], partner).wait_send())
    loop(1, cols, lambda i: col_wait(lax.rem(c + i, cols)).wait_send())
    loop(1, cols, lambda i: pcol_wait(lax.rem(c + i, cols)).wait_send())


def body(dims, kernel, labels, start_dual, penalty, box):
    hs, xs, ks, ys, ls = dims
    groups, rows, cols = hs * xs, hs * xs * ks, ys * ls
    height, width = kernel.shape
    settings = box.shape[0]
    piece = height // cols
    total = height * rows
    near_n, far_n = ys * ks, hs * xs * ls
    wide = 128 if height % 128 == 0 else height
    dma = pltpu.SemaphoreType.DMA
    vmem = pltpu.VMEM
    scratch = [
        vmem((height, width), BF16), vmem((height // wide, wide), jnp.int32), vmem((height, settings), F32),
        vmem((height, settings), F32), vmem((groups, ks, piece, settings), F32), dma((3,)),
        vmem((4, 2, piece, settings), F32), vmem((4, 2, piece, settings), F32), dma((4,)), dma((4,)),
        vmem((2, groups, piece, settings), BF16), vmem((2, groups, piece, settings), BF16), dma((2,)), dma((2,)),
        vmem((2, groups, piece, settings), BF16), vmem((2, groups, piece, settings), BF16), dma((2, groups)), dma((2, groups)),
        vmem((rows, piece, settings), BF16), dma((groups,)), dma((rows,)), dma((groups,)),
        vmem((cols, piece, settings), BF16), vmem((cols, piece, settings), BF16), dma((cols,)), dma((cols,)),
        vmem((cols, piece, settings), BF16), dma((cols,)), dma((cols,)),
        vmem((4, near_n, 2, settings), F32), dma((4, near_n)), dma((4, near_n)),
        vmem((4, far_n, 2, settings), F32), dma((4, far_n)), dma((4, far_n)),
    ]
    in_vmem = pl.BlockSpec(memory_space=vmem)
    in_hbm = pl.BlockSpec(memory_space=pltpu.HBM)
    dual, mult, gaps, offset = pl.pallas_call(
        functools.partial(admm, dims, total),
        out_shape=(
            jax.ShapeDtypeStruct((piece, settings), F32), jax.ShapeDtypeStruct((piece, settings), F32),
            jax.ShapeDtypeStruct((ITERS, settings), F32), jax.ShapeDtypeStruct((1, settings), F32),
        ),
        in_specs=[in_hbm, in_hbm, in_hbm, in_vmem, in_vmem],
        out_specs=(in_vmem,) * 4,
        scratch_shapes=scratch,
        compiler_params=pltpu.CompilerParams(collective_id=0, has_side_effects=True),
        name="admm",
    )(kernel, labels.reshape(height // wide, wide), start_dual, penalty[None, :], box[None, :])
    return dual, mult, gaps, offset[0]


def build(torus):
    dims = torus.devices.shape
    in_specs = (P(ROW, COL), P(ROW), P(ROW, None), P(), P())
    out_specs = (P(ROW_COL, None), P(ROW_COL, None), P(), P())
    return jax.shard_map(
        functools.partial(body, dims), mesh=torus, in_specs=in_specs, out_specs=out_specs, check_vma=False
    )


def solution(mesh):
    return build(Mesh(mesh.devices.reshape(4, 4, 2, 8, 2), ROW_COL))
```

```python
import functools

import jax
import jax.numpy as jnp
from jax import lax
from jax.experimental import pallas as pl
from jax.experimental.pallas import tpu as pltpu
from jax.sharding import Mesh
from jax.sharding import PartitionSpec as P

ITERS = 3
ROW = ("row_0", "row_1", "row_2")
COL = ("col_0", "col_1")
ROW_COL = ROW + COL
MESH = pl.DeviceIdType.MESH
F32 = jnp.float32
BF16 = jnp.bfloat16


def loop(low, high, step):
    def one(i, carry):
        step(i)
        return carry

    lax.fori_loop(low, high, one, jnp.int32(0))


def spread(count, step):
    def one(j):
        step(count // 2 + lax.div(j + 1, 2) * (2 * lax.rem(j, 2) - 1))

    loop(0, count - 1, one)


def remote(src, dst, send, recv, device):
    return pltpu.make_async_remote_copy(
        src_ref=src, dst_ref=dst, send_sem=send, recv_sem=recv, device_id=device, device_id_type=MESH
    )


def admm(
    dims, total,
    kernel_hbm, labels_hbm, start_hbm, penalty_hbm, box_hbm,
    dual_out, mult_out, gaps_out, offset_out,
    kernel_ref, labels_ref, start_ref, penalty_ref, box_ref, gaps_ref, offset_ref, signs_ref, part_ref, load_sem, store_sem,
    state_send, state_recv, state_ss, state_rs,
    core_send, core_recv, core_ss, core_rs,
    row_send, row_recv, row_ss, row_rs,
    gat_ref, gat_ss, gat_rs, fwd_ss,
    col_send, col_recv, col_ss, col_rs,
    pcol_ref, pcol_ss, pcol_rs,
    near_ref, near_ss, near_rs,
    far_ref, far_ss, far_rs,
    kcore_ref, kx_ref, kh_ref, ksum_ss, ksum_rs, ksum_send, ksum_recv, kmove_sem,
):
    hs, xs, ks, ys, ls = dims
    groups, rows, cols = hs * xs, hs * xs * ks, ys * ls
    h, x, k = (lax.axis_index(a) for a in ROW)
    y, l = (lax.axis_index(a) for a in COL)
    g = h * xs + x
    r = g * ks + k
    c = y * ls + l
    piece = state_send.shape[2]
    near_n, far_n = ys * ks, hs * xs * ls
    near_me = y * ks + k
    far_me = g * ls + l
    other = 1 - k

    def chip(to):
        return {"row_0": lax.div(to, xs), "row_1": lax.rem(to, xs)}

    def column(to):
        return {"col_0": lax.div(to, ls), "col_1": lax.rem(to, ls)}

    def whole(row, col):
        return {
            "row_0": lax.div(row, xs * ks), "row_1": lax.rem(lax.div(row, ks), xs), "row_2": lax.rem(row, ks),
            "col_0": lax.div(col, ls), "col_1": lax.rem(col, ls),
        }

    def near(to):
        return {"col_0": lax.div(to, ks), "row_2": lax.rem(to, ks)}

    def far(to):
        return {
            "row_0": lax.div(to, xs * ls), "row_1": lax.rem(lax.div(to, ls), xs), "col_1": lax.rem(to, ls)
        }

    partner = {"row_2": other}
    mine = g * ks + other
    block = r * cols + c
    to_piece = lax.rem(block, rows)
    to_column = whole(
        lax.div(to_piece, ks) * ks + (ks - 1 - lax.rem(to_piece, ks)), lax.div(block, rows)
    )
    owned = c * rows + mine
    to_row = whole(lax.div(owned, cols), lax.rem(owned, cols))

    load_k = pltpu.make_async_copy(kernel_hbm, kernel_ref, load_sem.at[0])
    load_s = pltpu.make_async_copy(start_hbm, start_ref, load_sem.at[1])
    load_l = pltpu.make_async_copy(labels_hbm, labels_ref, load_sem.at[2])
    load_p = pltpu.make_async_copy(penalty_hbm, penalty_ref, load_sem.at[3])
    load_b = pltpu.make_async_copy(box_hbm, box_ref, load_sem.at[4])
    load_l.start()
    load_b.start()
    load_s.start()
    load_p.start()
    load_k.start()

    barrier = pltpu.get_barrier_semaphore()

    def greet(device):
        pl.semaphore_signal(barrier, inc=1, device_id=device, device_id_type=MESH)

    greet(to_column)
    greet(to_row)
    loop(1, far_n, lambda i: greet(far(lax.rem(far_me + i, far_n))))
    loop(1, near_n, lambda i: greet(near(lax.rem(near_me + i, near_n))))
    crossed = ys * (ls - 1)
    if crossed:
        def cross(i):
            greet({"col_0": lax.rem(i, ys), "col_1": lax.rem(l + 1 + lax.div(i, ys), ls)})
        loop(0, crossed, cross)

    load_l.wait()
    wide = labels_ref.shape[1]
    for i in range(labels_ref.shape[0]):
        line = labels_ref[i : i + 1, :].astype(F32)
        if wide == 128:
            block_signs = jnp.transpose(jnp.broadcast_to(line, (128, 128)))
        else:
            block_signs = jnp.broadcast_to(jnp.transpose(line), (wide, 128))
        signs_ref[i * wide : (i + 1) * wide, :] = block_signs
    load_b.wait()
    load_s.wait()
    load_p.wait()
    penalty = penalty_ref[...]
    box = box_ref[...]
    first = jnp.minimum(jnp.maximum(start_ref[...], 0.0), box)
    start_ref[...] = first
    weighted = (signs_ref[...] * first).astype(BF16)
    own_rows = pl.ds(pl.multiple_of(c * piece, 8), piece)
    signs_row = signs_ref[own_rows, :]
    dual = start_ref[own_rows, :]
    mult = jnp.zeros_like(dual)
    state_send[0, 0] = dual
    state_send[0, 1] = signs_row

    def move_state(t, device):
        remote(state_send.at[t], state_recv.at[t], state_ss.at[t], state_rs.at[t], device).start()

    def arrived_state(t):
        remote(state_send.at[t], state_recv.at[t], state_ss.at[t], state_rs.at[t], to_row).wait_recv()
        return state_recv[t, 0], state_recv[t, 1]

    def near_copy(t, i):
        return remote(near_ref.at[t, near_me], near_ref.at[t, near_me], near_ss.at[t], near_rs.at[t], near(i))

    def near_all(t):
        rest = near_ref.at[t, pl.ds(0, near_n - 1)]
        return remote(rest, rest, near_ss.at[t], near_rs.at[t], partner)

    def far_copy(t, i):
        return remote(far_ref.at[t, far_me], far_ref.at[t, far_me], far_ss.at[t], far_rs.at[t], far(i))

    def far_all(t):
        rest = far_ref.at[t, pl.ds(0, far_n - 1)]
        return remote(rest, rest, far_ss.at[t], far_rs.at[t], partner)

    def sum_start(t, top, bottom):
        near_ref[t, near_me, 0:1, :] = top
        near_ref[t, near_me, 1:2, :] = bottom
        spread(near_n, lambda i: near_copy(t, lax.rem(near_me + i, near_n)).start())

    def sum_middle(t):
        near_all(t).wait_recv()
        far_ref[t, far_me] = jnp.sum(near_ref[t], axis=0)
        spread(far_n, lambda i: far_copy(t, lax.rem(far_me + i, far_n)).start())

    def sum_end(t):
        far_all(t).wait_recv()
        return jnp.sum(far_ref[t], axis=0)

    def ksum_copy(ref, slot, stage, device):
        return remote(ref.at[slot], ref.at[slot], ksum_ss.at[stage], ksum_rs.at[stage], device)

    def ksum_all(ref, stage):
        rest = ref.at[pl.ds(0, ref.shape[0] - 1)]
        return remote(rest, rest, ksum_ss.at[stage], ksum_rs.at[stage], partner)

    def ksum_x():
        ksum_all(kcore_ref, 0).wait_recv()
        kx_ref[x] = jnp.sum(kcore_ref[...], axis=0)
        loop(1, xs, lambda i: ksum_copy(kx_ref, x, 1, {"row_1": lax.rem(x + i, xs)}).start())

    def ksum_h():
        if xs > 1:
            ksum_all(kx_ref, 1).wait_recv()
        kh_ref[h] = jnp.sum(kx_ref[...], axis=0)
        loop(1, hs, lambda i: ksum_copy(kh_ref, h, 2, {"row_0": lax.rem(h + i, hs)}).start())

    def ksum_mine():
        ksum_all(kh_ref, 2).wait_recv()
        sums = jnp.sum(kh_ref[...], axis=0)
        shape = (piece, sums.shape[1])
        here = lax.broadcasted_iota(jnp.int32, shape, 1) == lax.broadcasted_iota(jnp.int32, shape, 0) + mine * piece
        return jnp.sum(jnp.where(here, sums, 0.0), axis=1, keepdims=True)

    def local_bias(dual, mult, signs, product_sum):
        steady = jnp.sum(signs * (dual - mult), axis=0, keepdims=True)
        return steady - (product_sum - jnp.sum(signs, axis=0, keepdims=True)) / penalty

    def update(q, dual, mult, signs, offset):
        w = dual - mult - (q - 1.0) / penalty
        hinge = jnp.maximum(0.0, 1.0 - q - signs * offset)
        gap = jnp.sum(dual * q - dual + box * hinge, axis=0, keepdims=True)
        x_value = w - signs * offset
        dual_next = jnp.minimum(jnp.maximum(x_value + mult, 0.0), box)
        return dual_next, mult + x_value - dual_next, gap

    def row_copy(s, i):
        return remote(row_send.at[s, i], row_recv.at[s, g], row_ss.at[s], row_rs.at[s], chip(i))

    def row_all(s):
        rest = pl.ds(0, groups - 1)
        return remote(row_send.at[s, rest], row_recv.at[s, rest], row_ss.at[s], row_rs.at[s], partner)

    def core_copy(s):
        return remote(core_send.at[s], core_recv.at[s], core_ss.at[s], core_rs.at[s], partner)

    def transposed_start(s, weighted):
        product = lax.dot_general(
            kernel_ref[...], weighted, (((0,), (0,)), ((), ())), preferred_element_type=F32
        )
        part_ref[...] = product.reshape(part_ref.shape)
        core_send[s] = part_ref[:, k].astype(BF16)
        return jnp.sum(product, axis=0, keepdims=True)

    def transposed_send(s):
        core_copy(s).wait_recv()
        both = part_ref[:, other] + core_recv[s].astype(F32)
        part_ref[:, other] = both
        row_send[s] = both.astype(BF16)
        spread(groups, lambda i: row_copy(s, lax.rem(g + i, groups)).start())

    def transposed_sum(s):
        row_recv[s, g] = jnp.zeros(row_recv.shape[2:], BF16)
        row_all(s).wait_recv()
        return part_ref[g, other] + jnp.sum(row_recv[s].astype(F32), axis=0)

    zero = jnp.zeros((1, box.shape[1]), F32)

    load_k.wait()
    product_sum = transposed_start(0, weighted)
    ones = jnp.ones((8, kernel_ref.shape[0]), BF16)
    kcore_ref[k] = jnp.dot(ones, kernel_ref[...], preferred_element_type=F32)[0:1]
    pl.semaphore_wait(barrier, 2 + far_n - 1 + near_n - 1 + crossed)
    core_copy(0).start()
    sum_start(0, local_bias(dual, mult, signs_row, product_sum), zero)
    ksum_copy(kcore_ref, k, 0, partner).start()
    move_state(0, to_column)
    transposed_send(0)
    ksum_x()
    sum_middle(0)
    ksum_h()
    q_sum = transposed_sum(0)
    dual, signs_col = arrived_state(0)
    mult = jnp.zeros_like(dual)
    ksum = ksum_mine()
    offset = sum_end(0)[0:1] / total
    dual, mult, gap = update(signs_col * q_sum, dual, mult, signs_col, offset)

    gat_ref[mine] = (signs_col * dual).astype(BF16)

    def gat_copy(slot, send, device):
        return remote(gat_ref.at[slot], gat_ref.at[slot], send, gat_rs.at[slot], device)

    spread(groups, lambda i: gat_copy(mine, gat_ss.at[0], chip(lax.rem(g + i, groups))).start())
    gat_copy(mine, fwd_ss.at[0], partner).start()
    weighted = gat_ref[mine].astype(F32)
    sum_start(1, local_bias(dual, mult, signs_col, jnp.sum(ksum * weighted, axis=0, keepdims=True)), gap)
    state_send[1, 0] = dual
    state_send[1, 1] = mult
    ksum_send[...] = jnp.broadcast_to(ksum, ksum_send.shape)
    move_state(1, to_row)
    move_ksum = remote(ksum_send, ksum_recv, kmove_sem.at[0], kmove_sem.at[1], to_row)
    move_ksum.start()

    def forward(i):
        slot = lax.rem(g + i, groups) * ks + other
        gat_copy(slot, fwd_ss.at[0], partner).wait_recv()
        gat_copy(slot, fwd_ss.at[0], partner).start()

    loop(1, groups, forward)
    sum_middle(1)
    loop(0, groups, lambda i: gat_copy(i * ks + k, fwd_ss.at[0], partner).wait_recv())
    gathered = gat_ref[...].astype(F32).reshape(rows * piece, -1).astype(BF16)
    product = jnp.dot(kernel_ref[...], gathered, preferred_element_type=F32)
    col_send[...] = product.reshape(col_send.shape).astype(BF16)
    part_ref[0 : cols // ks] = product.reshape(cols // ks, ks, piece, -1)

    def col_copy(i):
        return remote(col_send.at[i], col_recv.at[c], col_ss.at[0], col_rs.at[0], column(i))

    rest = pl.ds(0, cols - 1)
    col_all = remote(col_send.at[rest], col_recv.at[rest], col_ss.at[0], col_rs.at[0], partner)

    spread(cols, lambda i: col_copy(lax.rem(c + i, cols)).start())
    col_recv[c] = jnp.zeros(col_recv.shape[1:], BF16)
    col_all.wait_recv()
    q_sum = part_ref[lax.div(c, ks), lax.rem(c, ks)] + jnp.sum(col_recv[...].astype(F32), axis=0)
    dual, mult = arrived_state(1)
    sums = sum_end(1)
    gaps_ref[0:1, :] = sums[1:2] / total
    offset = sums[0:1] / total
    dual, mult, gap = update(signs_row * q_sum, dual, mult, signs_row, offset)

    pcol_ref[c] = (signs_row * dual).astype(BF16)

    def pcol_copy(i):
        return remote(pcol_ref.at[c], pcol_ref.at[c], pcol_ss.at[0], pcol_rs.at[0], column(i))

    pcol_all = remote(pcol_ref.at[rest], pcol_ref.at[rest], pcol_ss.at[0], pcol_rs.at[0], partner)
    spread(cols, lambda i: pcol_copy(lax.rem(c + i, cols)).start())
    move_ksum.wait_recv()
    weighted = pcol_ref[c].astype(F32)
    sum_start(2, local_bias(dual, mult, signs_row, jnp.sum(ksum_recv[...] * weighted, axis=0, keepdims=True)), gap)
    state_send[2, 0] = dual
    state_send[2, 1] = mult
    move_state(2, to_column)
    pcol_all.wait_recv()
    weighted = pcol_ref[...].astype(F32).reshape(cols * piece, -1).astype(BF16)
    transposed_start(1, weighted)
    core_copy(1).start()
    sum_middle(2)
    transposed_send(1)
    q_sum = transposed_sum(1)
    dual, mult = arrived_state(2)
    sums = sum_end(2)
    gaps_ref[1:2, :] = sums[1:2] / total
    offset = sums[0:1] / total
    dual, mult, gap = update(signs_col * q_sum, dual, mult, signs_col, offset)

    sum_start(3, zero, gap)
    state_send[3, 0] = dual
    state_send[3, 1] = mult
    move_state(3, to_row)
    offset_ref[...] = offset
    store_o = pltpu.make_async_copy(offset_ref, offset_out, store_sem.at[0])
    store_o.start()
    for t in range(3):
        remote(state_send.at[t], state_recv.at[t], state_ss.at[t], state_rs.at[t], to_row).wait_send()
        near_all(t).wait_send()
        far_all(t).wait_send()
    for s in range(2):
        core_copy(s).wait_send()
        row_all(s).wait_send()
    rest = pl.ds(0, groups - 1)
    remote(gat_ref.at[rest], gat_ref.at[rest], gat_ss.at[0], gat_rs.at[0], partner).wait_send()
    rest = pl.ds(0, groups)
    remote(gat_ref.at[rest], gat_ref.at[rest], fwd_ss.at[0], gat_rs.at[0], partner).wait_send()
    col_all.wait_send()
    pcol_all.wait_send()
    move_ksum.wait_send()
    ksum_all(kcore_ref, 0).wait_send()
    if xs > 1:
        ksum_all(kx_ref, 1).wait_send()
    ksum_all(kh_ref, 2).wait_send()
    sum_middle(3)
    remote(state_send.at[3], state_recv.at[3], state_ss.at[3], state_rs.at[3], to_row).wait()
    store_d = pltpu.make_async_copy(state_recv.at[3, 0], dual_out, store_sem.at[1])
    store_m = pltpu.make_async_copy(state_recv.at[3, 1], mult_out, store_sem.at[2])
    store_d.start()
    store_m.start()
    gaps_ref[2:3, :] = sum_end(3)[1:2] / total
    store_g = pltpu.make_async_copy(gaps_ref, gaps_out, store_sem.at[3])
    store_g.start()
    near_all(3).wait_send()
    far_all(3).wait_send()
    store_o.wait()
    store_d.wait()
    store_m.wait()
    store_g.wait()


def hand_over(*refs):
    half = len(refs) // 2
    for source, target in zip(refs[:half], refs[half:]):
        target[...] = source[...]


def body(dims, kernel, labels, start_dual, penalty, box):
    hs, xs, ks, ys, ls = dims
    groups, rows, cols = hs * xs, hs * xs * ks, ys * ls
    height, width = kernel.shape
    settings = box.shape[0]
    piece = height // cols
    total = height * rows
    near_n, far_n = ys * ks, hs * xs * ls
    wide = 128 if height % 128 == 0 else height
    dma = pltpu.SemaphoreType.DMA
    vmem = pltpu.VMEM
    scratch = [
        vmem((height, width), BF16), vmem((height // wide, wide), jnp.int32), vmem((height, settings), F32),
        vmem((1, settings), F32), vmem((1, settings), F32), vmem((ITERS, settings), F32), vmem((1, settings), F32),
        vmem((height, settings), F32), vmem((groups, ks, piece, settings), F32), dma((5,)), dma((4,)),
        vmem((4, 2, piece, settings), F32), vmem((4, 2, piece, settings), F32), dma((4,)), dma((4,)),
        vmem((2, groups, piece, settings), BF16), vmem((2, groups, piece, settings), BF16), dma((2,)), dma((2,)),
        vmem((2, groups, piece, settings), BF16), vmem((2, groups, piece, settings), BF16), dma((2,)), dma((2,)),
        vmem((rows, piece, settings), BF16), dma((1,)), dma((rows,)), dma((1,)),
        vmem((cols, piece, settings), BF16), vmem((cols, piece, settings), BF16), dma((1,)), dma((1,)),
        vmem((cols, piece, settings), BF16), dma((1,)), dma((1,)),
        vmem((4, near_n, 2, settings), F32), dma((4,)), dma((4,)),
        vmem((4, far_n, 2, settings), F32), dma((4,)), dma((4,)),
        vmem((ks, 1, width), F32), vmem((xs, 1, width), F32), vmem((hs, 1, width), F32), dma((3,)), dma((3,)),
        vmem((piece, settings), F32), vmem((piece, settings), F32), dma((2,)),
    ]
    in_vmem = pl.BlockSpec(memory_space=vmem)
    in_hbm = pl.BlockSpec(memory_space=pltpu.HBM)
    outs_shape = tuple(
        jax.ShapeDtypeStruct(shape, F32)
        for shape in ((piece, settings), (piece, settings), (ITERS, settings), (1, settings))
    )
    outs = pl.pallas_call(
        functools.partial(admm, dims, total),
        out_shape=outs_shape,
        in_specs=[in_hbm] * 5,
        out_specs=(in_hbm,) * 4,
        scratch_shapes=scratch,
        compiler_params=pltpu.CompilerParams(collective_id=0, has_side_effects=True),
        name="admm",
    )(kernel, labels.reshape(height // wide, wide), start_dual, penalty[None, :], box[None, :])
    dual, mult, gaps, offset = pl.pallas_call(
        hand_over, out_shape=outs_shape, in_specs=[in_vmem] * 4, out_specs=(in_vmem,) * 4, name="hand_over"
    )(*outs)
    return dual, mult, gaps, offset[0]


def build(torus):
    dims = torus.devices.shape
    in_specs = (P(ROW, COL), P(ROW), P(ROW, None), P(), P())
    out_specs = (P(ROW_COL, None), P(ROW_COL, None), P(), P())
    return jax.shard_map(
        functools.partial(body, dims), mesh=torus, in_specs=in_specs, out_specs=out_specs, check_vma=False
    )


def solution(mesh):
    return build(Mesh(mesh.devices.reshape(4, 4, 2, 8, 2), ROW_COL))
```

```python
import functools

import jax
import jax.numpy as jnp
from jax import lax
from jax.experimental import pallas as pl
from jax.experimental.pallas import tpu as pltpu
from jax.sharding import Mesh
from jax.sharding import PartitionSpec as P

ITERS = 3
ROW = ("row_0", "row_1", "row_2")
COL = ("col_0", "col_1")
ROW_COL = ROW + COL
MESH = pl.DeviceIdType.MESH
F32 = jnp.float32
BF16 = jnp.bfloat16
I16 = jnp.int16
LEVELS = 32767.0


def loop(low, high, step):
    def one(i, carry):
        step(i)
        return carry

    lax.fori_loop(low, high, one, jnp.int32(0))


def spread(count, step):
    def one(j):
        step(count // 2 + lax.div(j + 1, 2) * (2 * lax.rem(j, 2) - 1))

    loop(0, count - 1, one)


def flip(i):
    return i + 1 - 2 * lax.rem(i, 2)


def coded(values):
    most = jnp.maximum(jnp.max(jnp.max(jnp.abs(values), axis=0), axis=0, keepdims=True), 1e-30)
    return jnp.round(values * (LEVELS / most)).astype(jnp.int32).astype(I16), most / LEVELS


def decoded_sum(codes, scales):
    return jnp.sum(codes.astype(jnp.int32).astype(F32) * scales, axis=0)


def write_signs(labels_ref, signs_ref):
    wide = labels_ref.shape[1]
    for i in range(labels_ref.shape[0]):
        line = labels_ref[i : i + 1, :].astype(F32)
        if wide == 128:
            block_signs = jnp.transpose(jnp.broadcast_to(line, (128, 128)))
        else:
            block_signs = jnp.broadcast_to(jnp.transpose(line), (wide, 128))
        signs_ref[i * wide : (i + 1) * wide, :] = block_signs


def remote(src, dst, send, recv, device):
    return pltpu.make_async_remote_copy(
        src_ref=src, dst_ref=dst, send_sem=send, recv_sem=recv, device_id=device, device_id_type=MESH
    )


def admm(
    dims, total,
    kernel_hbm, labels_hbm, start_hbm, penalty_hbm, box_hbm,
    dual_out, mult_out, gaps_out, offset_out,
    kernel_ref, labels_ref, start_ref, penalty_ref, box_ref, dual_ref, mult_ref, gaps_ref, offset_ref, signs_ref, part_ref,
    load_sem, store_sem,
    first_ref, first_labels_ref, first_signs_ref, first_ss, first_rs,
    state_send, state_recv, state_ss, state_rs,
    core_recv, core_ss, core_rs,
    row_send, row_recv, row_ss, row_rs, rscale_send, rscale_recv, rscale_ss, rscale_rs,
    gat_ref, gat_ss, gat_rs, fwd_ss,
    col_send, col_recv, col_ss, col_rs, cscale_send, cscale_recv, cscale_ss, cscale_rs,
    pcol_ref, pcol_ss, pcol_rs,
    near_ref, near_ss, near_rs,
    far_ref, far_ss, far_rs,
    kcore_ref, kx_ref, kh_ref, ksum_ss, ksum_rs, ksum_send, ksum_recv, kmove_sem,
):
    hs, xs, ks, ys, ls = dims
    groups, rows, cols = hs * xs, hs * xs * ks, ys * ls
    h, x, k = (lax.axis_index(a) for a in ROW)
    y, l = (lax.axis_index(a) for a in COL)
    g = h * xs + x
    r = g * ks + k
    c = y * ls + l
    piece, settings = state_send.shape[1:]
    half = groups * piece
    near_n, far_n = ys * ks, hs * xs * ls
    near_me = y * ks + k
    far_me = g * ls + l
    other = 1 - k

    def chip(to):
        return {"row_0": lax.div(to, xs), "row_1": lax.rem(to, xs)}

    def column(to):
        return {"col_0": lax.div(to, ls), "col_1": lax.rem(to, ls)}

    def whole(row, col):
        return {
            "row_0": lax.div(row, xs * ks), "row_1": lax.rem(lax.div(row, ks), xs), "row_2": lax.rem(row, ks),
            "col_0": lax.div(col, ls), "col_1": lax.rem(col, ls),
        }

    def near(to):
        return {"col_0": lax.div(to, ks), "row_2": lax.rem(to, ks)}

    def far(to):
        return {
            "row_0": lax.div(to, xs * ls), "row_1": lax.rem(lax.div(to, ls), xs), "col_1": lax.rem(to, ls)
        }

    partner = {"row_2": other}
    spot = flip(g)
    mine = k * groups + spot
    block = r * cols + c
    to_piece = lax.rem(block, rows)
    to_column = whole(
        flip(lax.rem(to_piece, groups)) * ks + lax.div(to_piece, groups), lax.div(block, rows)
    )
    owned = c * rows + mine
    to_row = whole(lax.div(owned, cols), lax.rem(owned, cols))

    load_k = pltpu.make_async_copy(kernel_hbm, kernel_ref, load_sem.at[0])
    load_s = pltpu.make_async_copy(start_hbm, start_ref, load_sem.at[1])
    load_l = pltpu.make_async_copy(labels_hbm, labels_ref, load_sem.at[2])
    load_p = pltpu.make_async_copy(penalty_hbm, penalty_ref, load_sem.at[3])
    load_b = pltpu.make_async_copy(box_hbm, box_ref, load_sem.at[4])
    load_l.start()
    load_b.start()
    load_s.start()
    load_p.start()
    load_k.start()

    barrier = pltpu.get_barrier_semaphore()

    def greet(device):
        pl.semaphore_signal(barrier, inc=1, device_id=device, device_id_type=MESH)

    loop(1, far_n, lambda i: greet(far(lax.rem(far_me + i, far_n))))
    loop(1, near_n, lambda i: greet(near(lax.rem(near_me + i, near_n))))
    crossed = ys * (ls - 1)
    if crossed:
        def cross(i):
            greet({"col_0": lax.rem(i, ys), "col_1": lax.rem(l + 1 + lax.div(i, ys), ls)})
        loop(0, crossed, cross)

    load_l.wait()
    write_signs(labels_ref, signs_ref)
    load_b.wait()
    load_s.wait()
    load_p.wait()
    penalty = penalty_ref[...]
    box = box_ref[...]
    def clipped(values):
        return jnp.minimum(jnp.maximum(values, 0.0), box)

    weighted = (signs_ref[...] * clipped(start_ref[...])).astype(BF16)
    own_rows = pl.ds(pl.multiple_of(c * piece, 8), piece)
    signs_row = signs_ref[own_rows, :]
    dual = clipped(start_ref[own_rows, :])
    mult = jnp.zeros_like(dual)

    from_here = lax.div(g, ls) == y
    to_side = lax.rem(g, ls)
    local = jnp.logical_and(g == c, lax.rem(spot, ls) == l)

    def first_copies(j, device):
        rows_j = pl.ds(pl.multiple_of(j * piece, 8), piece)
        return (
            remote(start_ref.at[rows_j], first_ref, first_ss.at[0, lax.div(j, ls)], first_rs.at[0], device),
            remote(labels_ref, first_labels_ref, first_ss.at[1, lax.div(j, ls)], first_rs.at[1], device),
        )

    def first_each(act):
        def one(i):
            j = i * ls + l
            to = flip(j)

            @pl.when(jnp.logical_not(jnp.logical_and(to == g, to_side == l)))
            def _():
                device = {"row_0": lax.div(to, xs), "row_1": lax.rem(to, xs), "col_1": to_side}
                for copy in first_copies(j, device):
                    act(copy)

        @pl.when(from_here)
        def _():
            loop(0, groups // ls, one)

    def first_arrived():
        @pl.when(jnp.logical_not(local))
        def _():
            for copy in first_copies(0, partner):
                copy.wait_recv()

        @pl.when(local)
        def _():
            first_ref[...] = start_ref[pl.ds(pl.multiple_of(spot * piece, 8), piece), :]
            first_labels_ref[...] = labels_ref[...]

        write_signs(first_labels_ref, first_signs_ref)
        return clipped(first_ref[...]), first_signs_ref[pl.ds(pl.multiple_of(spot * piece, 8), piece), :]

    def state_copy(t, device):
        return remote(state_send.at[t], state_recv.at[t], state_ss.at[t], state_rs.at[t], device)

    def move_state(t, state, device):
        state_send[t] = state
        state_copy(t, device).start()

    def arrived_state(t):
        state_copy(t, to_row).wait_recv()
        state = state_recv[t]
        return clipped(state), state - clipped(state)

    def near_copy(t, i):
        return remote(near_ref.at[t, near_me], near_ref.at[t, near_me], near_ss.at[t], near_rs.at[t], near(i))

    def near_all(t):
        rest = near_ref.at[t, pl.ds(0, near_n - 1)]
        return remote(rest, rest, near_ss.at[t], near_rs.at[t], partner)

    def far_copy(t, i):
        return remote(far_ref.at[t, far_me], far_ref.at[t, far_me], far_ss.at[t], far_rs.at[t], far(i))

    def far_all(t):
        rest = far_ref.at[t, pl.ds(0, far_n - 1)]
        return remote(rest, rest, far_ss.at[t], far_rs.at[t], partner)

    def sum_start(t, top, bottom):
        near_ref[t, near_me, 0:1, :] = top
        near_ref[t, near_me, 1:2, :] = bottom
        spread(near_n, lambda i: near_copy(t, lax.rem(near_me + i, near_n)).start())

    def sum_middle(t):
        near_all(t).wait_recv()
        far_ref[t, far_me] = jnp.sum(near_ref[t], axis=0)
        spread(far_n, lambda i: far_copy(t, lax.rem(far_me + i, far_n)).start())

    def sum_end(t):
        far_all(t).wait_recv()
        return jnp.sum(far_ref[t], axis=0)

    def ksum_copy(ref, slot, stage, device):
        return remote(ref.at[slot], ref.at[slot], ksum_ss.at[stage], ksum_rs.at[stage], device)

    def ksum_all(ref, stage):
        rest = ref.at[pl.ds(0, ref.shape[0] - 1)]
        return remote(rest, rest, ksum_ss.at[stage], ksum_rs.at[stage], partner)

    def ksum_x():
        ksum_all(kcore_ref, 0).wait_recv()
        kx_ref[x] = jnp.sum(kcore_ref[...], axis=0)
        loop(1, xs, lambda i: ksum_copy(kx_ref, x, 1, {"row_1": lax.rem(x + i, xs)}).start())

    def ksum_h():
        if xs > 1:
            ksum_all(kx_ref, 1).wait_recv()
        kh_ref[h] = jnp.sum(kx_ref[...], axis=0)
        loop(1, hs, lambda i: ksum_copy(kh_ref, h, 2, {"row_0": lax.rem(h + i, hs)}).start())

    def ksum_row():
        ksum_all(kh_ref, 2).wait_recv()
        return jnp.sum(kh_ref[...], axis=0)

    def ksum_of(sums, at):
        shape = (piece, sums.shape[1])
        here = lax.broadcasted_iota(jnp.int32, shape, 1) == lax.broadcasted_iota(jnp.int32, shape, 0) + at * piece
        return jnp.sum(jnp.where(here, sums, 0.0), axis=1, keepdims=True)

    def local_bias(dual, mult, signs, product_sum):
        steady = jnp.sum(signs * (dual - mult), axis=0, keepdims=True)
        return steady - (product_sum - jnp.sum(signs, axis=0, keepdims=True)) / penalty

    def update(q, dual, mult, signs, offset):
        w = dual - mult - (q - 1.0) / penalty
        hinge = jnp.maximum(0.0, 1.0 - q - signs * offset)
        gap = jnp.sum(dual * q - dual + box * hinge, axis=0, keepdims=True)
        x_value = w - signs * offset
        state = x_value + mult
        return state, clipped(state), state - clipped(state), gap

    def row_copies(s, i):
        j = flip(i)
        return (
            remote(row_send.at[s, j], row_recv.at[s, g], row_ss.at[s], row_rs.at[s], chip(i)),
            remote(rscale_send.at[s], rscale_recv.at[s, g], rscale_ss.at[s], rscale_rs.at[s], chip(i)),
        )

    def row_all(s):
        rest = pl.ds(0, groups - 1)
        return (
            remote(row_send.at[s, rest], row_recv.at[s, rest], row_ss.at[s], row_rs.at[s], partner),
            remote(rscale_recv.at[s, rest], rscale_recv.at[s, rest], rscale_ss.at[s], rscale_rs.at[s], partner),
        )

    def core_copy(s):
        return remote(part_ref.at[other], core_recv.at[s], core_ss.at[s], core_rs.at[s], partner)

    def transposed_half(which, weighted):
        columns = pl.ds(pl.multiple_of(which * half, 128) if half % 128 == 0 else which * half, half)
        product = lax.dot_general(
            kernel_ref[:, columns], weighted, (((0,), (0,)), ((), ())), preferred_element_type=F32
        )
        part_ref[which] = product.reshape(part_ref.shape[1:])
        return jnp.sum(product, axis=0, keepdims=True)

    def transposed_send(s):
        core_copy(s).wait_recv()
        both = part_ref[k] + core_recv[s]
        part_ref[k] = both
        row_send[s], rscale_send[s] = coded(both)

        def send(i):
            for copy in row_copies(s, lax.rem(g + i, groups)):
                copy.start()

        spread(groups, send)

    def transposed_sum(s):
        row_recv[s, g] = jnp.zeros(row_recv.shape[2:], I16)
        rscale_recv[s, g] = jnp.zeros(rscale_recv.shape[2:], F32)
        for copy in row_all(s):
            copy.wait_recv()
        return part_ref[k, spot] + decoded_sum(row_recv[s], rscale_recv[s])

    zero = jnp.zeros((1, box.shape[1]), F32)

    load_k.wait()
    far_sum = transposed_half(other, weighted)
    pl.semaphore_wait(barrier, far_n - 1 + near_n - 1 + crossed)
    core_copy(0).start()
    product_sum = far_sum + transposed_half(k, weighted)
    ones = jnp.ones((8, kernel_ref.shape[0]), BF16)
    kcore_ref[k] = jnp.dot(ones, kernel_ref[...], preferred_element_type=F32)[0:1]
    sum_start(0, local_bias(dual, mult, signs_row, product_sum), zero)
    ksum_copy(kcore_ref, k, 0, partner).start()
    transposed_send(0)
    first_each(lambda copy: copy.start())
    ksum_x()
    sum_middle(0)
    ksum_h()
    q_sum = transposed_sum(0)
    core_copy(0).wait_send()
    dual, signs_col = first_arrived()
    mult = jnp.zeros_like(dual)
    ksum_send[...] = ksum_row()
    ksum = ksum_of(ksum_send[...], mine)
    offset = sum_end(0)[0:1] / total
    state, dual, mult, gap = update(signs_col * q_sum, dual, mult, signs_col, offset)

    gat_ref[mine] = (signs_col * dual).astype(BF16)

    def gat_copy(slot, send, device):
        return remote(gat_ref.at[slot], gat_ref.at[slot], send, gat_rs.at[slot], device)

    spread(groups, lambda i: gat_copy(mine, gat_ss.at[0], chip(lax.rem(g + i, groups))).start())
    gat_copy(mine, fwd_ss.at[0], partner).start()
    weighted = gat_ref[mine].astype(F32)
    sum_start(1, local_bias(dual, mult, signs_col, jnp.sum(ksum * weighted, axis=0, keepdims=True)), gap)
    move_state(0, state, to_row)
    move_ksum = remote(ksum_send, ksum_recv, kmove_sem.at[0], kmove_sem.at[1], to_row)
    move_ksum.start()

    def forward(i):
        slot = k * groups + flip(lax.rem(g + i, groups))
        gat_copy(slot, fwd_ss.at[0], partner).wait_recv()
        gat_copy(slot, fwd_ss.at[0], partner).start()

    loop(1, groups, forward)
    sum_middle(1)
    loop(0, groups, lambda i: gat_copy(other * groups + i, fwd_ss.at[0], partner).wait_recv())
    gathered = gat_ref[...].astype(F32).reshape(rows * piece, -1).astype(BF16)
    product = jnp.dot(kernel_ref[...], gathered, preferred_element_type=F32)
    product = product.reshape(cols, piece, settings)
    col_send[...], cscale_send[...] = coded(product)
    part_ref[0] = product

    def col_copies(i):
        return (
            remote(col_send.at[i], col_recv.at[c], col_ss.at[0], col_rs.at[0], column(i)),
            remote(cscale_send, cscale_recv.at[c], cscale_ss.at[0], cscale_rs.at[0], column(i)),
        )

    def col_start(i):
        for copy in col_copies(lax.rem(c + i, cols)):
            copy.start()

    rest = pl.ds(0, cols - 1)
    col_all = (
        remote(col_send.at[rest], col_recv.at[rest], col_ss.at[0], col_rs.at[0], partner),
        remote(cscale_recv.at[rest], cscale_recv.at[rest], cscale_ss.at[0], cscale_rs.at[0], partner),
    )

    spread(cols, col_start)
    col_recv[c] = jnp.zeros(col_recv.shape[1:], I16)
    cscale_recv[c] = jnp.zeros(cscale_recv.shape[1:], F32)
    for copy in col_all:
        copy.wait_recv()
    q_sum = part_ref[0, c] + decoded_sum(col_recv[...], cscale_recv[...])
    dual, mult = arrived_state(0)
    sums = sum_end(1)
    gaps_ref[0:1, :] = sums[1:2] / total
    offset = sums[0:1] / total
    state, dual, mult, gap = update(signs_row * q_sum, dual, mult, signs_row, offset)

    pcol_ref[c] = (signs_row * dual).astype(BF16)

    def pcol_copy(i):
        return remote(pcol_ref.at[c], pcol_ref.at[c], pcol_ss.at[0], pcol_rs.at[0], column(i))

    pcol_all = remote(pcol_ref.at[rest], pcol_ref.at[rest], pcol_ss.at[0], pcol_rs.at[0], partner)
    spread(cols, lambda i: pcol_copy(lax.rem(c + i, cols)).start())
    move_ksum.wait_recv()
    weighted = pcol_ref[c].astype(F32)
    ksum = ksum_of(ksum_recv[...], lax.rem(block, rows))
    sum_start(2, local_bias(dual, mult, signs_row, jnp.sum(ksum * weighted, axis=0, keepdims=True)), gap)
    move_state(1, state, to_column)
    pcol_all.wait_recv()
    weighted = pcol_ref[...].astype(F32).reshape(cols * piece, -1).astype(BF16)
    transposed_half(other, weighted)
    core_copy(1).start()
    transposed_half(k, weighted)
    sum_middle(2)
    transposed_send(1)
    q_sum = transposed_sum(1)
    dual, mult = arrived_state(1)
    sums = sum_end(2)
    gaps_ref[1:2, :] = sums[1:2] / total
    offset = sums[0:1] / total
    state, dual, mult, gap = update(signs_col * q_sum, dual, mult, signs_col, offset)

    sum_start(3, zero, gap)
    move_state(2, state, to_row)
    offset_ref[...] = offset
    store_o = pltpu.make_async_copy(offset_ref, offset_out, store_sem.at[0])
    store_o.start()
    for t in range(3):
        near_all(t).wait_send()
        far_all(t).wait_send()
    state_copy(0, to_row).wait_send()
    state_copy(1, to_row).wait_send()
    core_copy(1).wait_send()
    for copy in row_all(0) + row_all(1) + col_all:
        copy.wait_send()
    first_each(lambda copy: copy.wait_send())
    rest = pl.ds(0, groups - 1)
    remote(gat_ref.at[rest], gat_ref.at[rest], gat_ss.at[0], gat_rs.at[0], partner).wait_send()
    rest = pl.ds(0, groups)
    remote(gat_ref.at[rest], gat_ref.at[rest], fwd_ss.at[0], gat_rs.at[0], partner).wait_send()
    pcol_all.wait_send()
    move_ksum.wait_send()
    ksum_all(kcore_ref, 0).wait_send()
    if xs > 1:
        ksum_all(kx_ref, 1).wait_send()
    ksum_all(kh_ref, 2).wait_send()
    sum_middle(3)
    state_copy(2, to_row).wait_send()
    dual_ref[...], mult_ref[...] = arrived_state(2)
    store_d = pltpu.make_async_copy(dual_ref, dual_out, store_sem.at[1])
    store_m = pltpu.make_async_copy(mult_ref, mult_out, store_sem.at[2])
    store_d.start()
    store_m.start()
    gaps_ref[2:3, :] = sum_end(3)[1:2] / total
    store_g = pltpu.make_async_copy(gaps_ref, gaps_out, store_sem.at[3])
    store_g.start()
    near_all(3).wait_send()
    far_all(3).wait_send()
    store_o.wait()
    store_d.wait()
    store_m.wait()
    store_g.wait()


def hand_over(*refs):
    half = len(refs) // 2
    for source, target in zip(refs[:half], refs[half:]):
        target[...] = source[...]


def body(dims, kernel, labels, start_dual, penalty, box):
    hs, xs, ks, ys, ls = dims
    groups, rows, cols = hs * xs, hs * xs * ks, ys * ls
    height, width = kernel.shape
    settings = box.shape[0]
    piece = height // cols
    total = height * rows
    near_n, far_n = ys * ks, hs * xs * ls
    wide = 128 if height % 128 == 0 else height
    dma = pltpu.SemaphoreType.DMA
    vmem = pltpu.VMEM
    scratch = [
        vmem((height, width), BF16), vmem((height // wide, wide), jnp.int32), vmem((height, settings), F32),
        vmem((1, settings), F32), vmem((1, settings), F32), vmem((piece, settings), F32), vmem((piece, settings), F32),
        vmem((ITERS, settings), F32), vmem((1, settings), F32), vmem((height, settings), F32),
        vmem((ks, groups, piece, settings), F32), dma((5,)), dma((4,)),
        vmem((piece, settings), F32), vmem((height // wide, wide), jnp.int32), vmem((height, settings), F32), dma((2, groups // ls)), dma((2,)),
        vmem((3, piece, settings), F32), vmem((3, piece, settings), F32), dma((3,)), dma((3,)),
        vmem((2, groups, piece, settings), F32), dma((2,)), dma((2,)),
        vmem((2, groups, piece, settings), I16), vmem((2, groups, piece, settings), I16), dma((2,)), dma((2,)),
        vmem((2, 1, settings), F32), vmem((2, groups, 1, settings), F32), dma((2,)), dma((2,)),
        vmem((rows, piece, settings), BF16), dma((1,)), dma((rows,)), dma((1,)),
        vmem((cols, piece, settings), I16), vmem((cols, piece, settings), I16), dma((1,)), dma((1,)),
        vmem((1, settings), F32), vmem((cols, 1, settings), F32), dma((1,)), dma((1,)),
        vmem((cols, piece, settings), BF16), dma((1,)), dma((1,)),
        vmem((4, near_n, 2, settings), F32), dma((4,)), dma((4,)),
        vmem((4, far_n, 2, settings), F32), dma((4,)), dma((4,)),
        vmem((ks, 1, width), F32), vmem((xs, 1, width), F32), vmem((hs, 1, width), F32), dma((3,)), dma((3,)),
        vmem((1, width), F32), vmem((1, width), F32), dma((2,)),
    ]
    in_vmem = pl.BlockSpec(memory_space=vmem)
    in_hbm = pl.BlockSpec(memory_space=pltpu.HBM)
    outs_shape = tuple(
        jax.ShapeDtypeStruct(shape, F32)
        for shape in ((piece, settings), (piece, settings), (ITERS, settings), (1, settings))
    )
    outs = pl.pallas_call(
        functools.partial(admm, dims, total),
        out_shape=outs_shape,
        in_specs=[in_hbm] * 5,
        out_specs=(in_hbm,) * 4,
        scratch_shapes=scratch,
        compiler_params=pltpu.CompilerParams(collective_id=0, has_side_effects=True),
        name="admm",
    )(kernel, labels.reshape(height // wide, wide), start_dual, penalty[None, :], box[None, :])
    dual, mult, gaps, offset = pl.pallas_call(
        hand_over, out_shape=outs_shape, in_specs=[in_vmem] * 4, out_specs=(in_vmem,) * 4, name="hand_over"
    )(*outs)
    return dual, mult, gaps, offset[0]


def build(torus):
    dims = torus.devices.shape
    in_specs = (P(ROW, COL), P(ROW), P(ROW, None), P(), P())
    out_specs = (P(ROW_COL, None), P(ROW_COL, None), P(), P())
    return jax.shard_map(
        functools.partial(body, dims), mesh=torus, in_specs=in_specs, out_specs=out_specs, check_vma=False
    )


def solution(mesh):
    return build(Mesh(mesh.devices.reshape(4, 4, 2, 8, 2), ROW_COL))
```

```python
import functools

import jax
import jax.numpy as jnp
from jax import lax
from jax.experimental import pallas as pl
from jax.experimental.pallas import tpu as pltpu
from jax.sharding import Mesh
from jax.sharding import PartitionSpec as P

ITERS = 3
ROW = ("row_0", "row_1", "row_2")
COL = ("col_0", "col_1")
ROW_COL = ROW + COL
MESH = pl.DeviceIdType.MESH
F32 = jnp.float32
BF16 = jnp.bfloat16
I16 = jnp.int16
LEVELS = 32767.0


def loop(low, high, step):
    def one(i, carry):
        step(i)
        return carry

    lax.fori_loop(low, high, one, jnp.int32(0))


def spread(count, step):
    def one(j):
        step(count // 2 + lax.div(j + 1, 2) * (2 * lax.rem(j, 2) - 1))

    loop(0, count - 1, one)


def flip(i):
    return i + 1 - 2 * lax.rem(i, 2)


def coded(values):
    most = jnp.maximum(jnp.max(jnp.max(jnp.abs(values), axis=0), axis=0, keepdims=True), 1e-30)
    return jnp.round(values * (LEVELS / most)).astype(jnp.int32).astype(I16), most / LEVELS


def decoded_sum(codes, scales):
    return jnp.sum(codes.astype(jnp.int32).astype(F32) * scales, axis=0)


def write_signs(labels_ref, signs_ref):
    wide = labels_ref.shape[1]
    for i in range(labels_ref.shape[0]):
        line = labels_ref[i : i + 1, :].astype(F32)
        if wide == 128:
            block_signs = jnp.transpose(jnp.broadcast_to(line, (128, 128)))
        else:
            block_signs = jnp.broadcast_to(jnp.transpose(line), (wide, 128))
        signs_ref[i * wide : (i + 1) * wide, :] = block_signs


def remote(src, dst, send, recv, device):
    return pltpu.make_async_remote_copy(
        src_ref=src, dst_ref=dst, send_sem=send, recv_sem=recv, device_id=device, device_id_type=MESH
    )


def admm(
    dims, total,
    kernel_hbm, labels_hbm, start_hbm, penalty_hbm, box_hbm,
    dual_out, mult_out, gaps_out, offset_out,
    kernel_ref, turned_ref, weighted_ref, labels_ref, start_ref, penalty_ref, box_ref, signs_ref, part_ref,
    load_sem,
    first_ref, first_labels_ref, first_signs_ref, first_ss, first_rs,
    state_send, state_recv, state_ss, state_rs,
    core_recv, core_ss, core_rs,
    row_send, row_recv, row_ss, row_rs, rscale_send, rscale_recv, rscale_ss, rscale_rs,
    gat_ref, gat_ss, gat_rs, fwd_ss,
    col_send, col_recv, col_ss, col_rs, cscale_send, cscale_recv, cscale_ss, cscale_rs,
    pcol_ref, pcol_ss, pcol_rs,
    near_ref, near_ss, near_rs,
    far_ref, far_ss, far_rs,
    kcore_ref, kx_ref, kh_ref, ksum_ss, ksum_rs, ksum_send, ksum_recv, kmove_sem,
):
    hs, xs, ks, ys, ls = dims
    groups, rows, cols = hs * xs, hs * xs * ks, ys * ls
    h, x, k = (lax.axis_index(a) for a in ROW)
    y, l = (lax.axis_index(a) for a in COL)
    g = h * xs + x
    r = g * ks + k
    c = y * ls + l
    piece, settings = state_send.shape[1:]
    half = groups * piece
    near_n, far_n = ys * ks, hs * xs * ls
    near_me = k * ys + y
    far_me = l * groups + g
    other = 1 - k

    def chip(to):
        return {"row_0": lax.div(to, xs), "row_1": lax.rem(to, xs)}

    def column(to):
        return {"col_0": lax.div(to, ls), "col_1": lax.rem(to, ls)}

    def whole(row, col):
        return {
            "row_0": lax.div(row, xs * ks), "row_1": lax.rem(lax.div(row, ks), xs), "row_2": lax.rem(row, ks),
            "col_0": lax.div(col, ls), "col_1": lax.rem(col, ls),
        }

    def near(to):
        return {"row_2": lax.div(to, ys), "col_0": lax.rem(to, ys)}

    def far(to):
        on = lax.rem(to, groups)
        return {"row_0": lax.div(on, xs), "row_1": lax.rem(on, xs), "col_1": lax.div(to, groups)}

    partner = {"row_2": other}
    spot = flip(g)
    mine = k * groups + spot
    block = r * cols + c
    to_piece = lax.rem(block, rows)
    to_column = whole(
        flip(lax.rem(to_piece, groups)) * ks + lax.div(to_piece, groups), lax.div(block, rows)
    )
    owned = c * rows + mine
    to_row = whole(lax.div(owned, cols), lax.rem(owned, cols))

    load_k = pltpu.make_async_copy(kernel_hbm, kernel_ref, load_sem.at[0])
    load_s = pltpu.make_async_copy(start_hbm, start_ref, load_sem.at[1])
    load_l = pltpu.make_async_copy(labels_hbm, labels_ref, load_sem.at[2])
    load_p = pltpu.make_async_copy(penalty_hbm, penalty_ref, load_sem.at[3])
    load_b = pltpu.make_async_copy(box_hbm, box_ref, load_sem.at[4])
    load_l.start()
    load_b.start()
    load_s.start()
    load_p.start()
    load_k.start()

    barrier = pltpu.get_barrier_semaphore()

    def greet(device):
        pl.semaphore_signal(barrier, inc=1, device_id=device, device_id_type=MESH)

    spread(far_n, lambda i: greet(far(lax.rem(far_me + i, far_n))))
    loop(1, near_n, lambda i: greet(near(lax.rem(near_me + i, near_n))))
    crossed = ys * (ls - 1)
    if crossed:
        def cross(i):
            greet({"col_0": lax.rem(i, ys), "col_1": lax.rem(l + 1 + lax.div(i, ys), ls)})
        loop(0, crossed, cross)

    load_l.wait()
    write_signs(labels_ref, signs_ref)
    load_b.wait()
    load_s.wait()
    load_p.wait()
    penalty = penalty_ref[...]
    box = box_ref[...]
    def clipped(values):
        return jnp.minimum(jnp.maximum(values, 0.0), box)

    weighted_ref[0 : start_ref.shape[0], :] = (signs_ref[...] * clipped(start_ref[...])).astype(BF16)
    own_rows = pl.ds(pl.multiple_of(c * piece, 8), piece)
    signs_row = signs_ref[own_rows, :]
    dual = clipped(start_ref[own_rows, :])
    mult = jnp.zeros_like(dual)
    zero = jnp.zeros((1, settings), F32)

    from_here = lax.div(g, ls) == y
    to_side = lax.rem(g, ls)

    def first_copies(j, device):
        rows_j = pl.ds(pl.multiple_of(j * piece, 8), piece)
        return (
            remote(start_ref.at[rows_j], first_ref, first_ss.at[0], first_rs.at[0], device),
            remote(labels_ref, first_labels_ref, first_ss.at[1 + lax.div(j, ls)], first_rs.at[1], device),
        )

    def first_start():
        def one(i):
            j = i * ls + l
            for copy in first_copies(j, chip(flip(j)) | {"col_1": to_side}):
                copy.start()

        @pl.when(from_here)
        def _():
            loop(0, groups // ls, one)

    def first_sent():
        @pl.when(from_here)
        def _():
            sent = start_ref.at[pl.ds(0, groups // ls * piece)]
            remote(sent, sent, first_ss.at[0], first_rs.at[0], partner).wait_send()
            loop(0, groups // ls, lambda i: first_copies(i * ls + l, partner)[1].wait_send())

    def first_arrived():
        for copy in first_copies(0, partner):
            copy.wait_recv()
        write_signs(first_labels_ref, first_signs_ref)
        return clipped(first_ref[...]), first_signs_ref[pl.ds(pl.multiple_of(spot * piece, 8), piece), :]

    def state_copy(t, device):
        return remote(state_send.at[t], state_recv.at[t], state_ss.at[t], state_rs.at[t], device)

    def move_state(t, state, device):
        state_send[t] = state
        state_copy(t, device).start()

    def arrived_state(t):
        state_copy(t, to_row).wait_recv()
        state = state_recv[t]
        return clipped(state), state - clipped(state)

    def near_copy(t, i):
        return remote(near_ref.at[t, near_me], near_ref.at[t, near_me], near_ss.at[t], near_rs.at[t], near(i))

    def near_all(t):
        rest = near_ref.at[t, pl.ds(0, near_n - 1)]
        return remote(rest, rest, near_ss.at[t], near_rs.at[t], partner)

    def far_copy(t, i):
        return remote(far_ref.at[t, far_me], far_ref.at[t, far_me], far_ss.at[t], far_rs.at[t], far(i))

    def far_all(t):
        rest = far_ref.at[t, pl.ds(0, far_n - 1)]
        return remote(rest, rest, far_ss.at[t], far_rs.at[t], partner)

    def sum_start(t, top, bottom):
        near_ref[t, near_me, 0:1, :] = top
        near_ref[t, near_me, 1:2, :] = bottom
        spread(near_n, lambda i: near_copy(t, lax.rem(near_me + i, near_n)).start())

    def sum_middle(t):
        near_all(t).wait_recv()
        far_ref[t, far_me] = jnp.sum(near_ref[t], axis=0)
        spread(far_n, lambda i: far_copy(t, lax.rem(far_me + i, far_n)).start())

    def sum_end(t):
        far_all(t).wait_recv()
        return jnp.sum(far_ref[t], axis=0)

    def ksum_copy(ref, slot, stage, device):
        return remote(ref.at[slot], ref.at[slot], ksum_ss.at[stage], ksum_rs.at[stage], device)

    def ksum_all(ref, stage):
        rest = ref.at[pl.ds(0, ref.shape[0] - 1)]
        return remote(rest, rest, ksum_ss.at[stage], ksum_rs.at[stage], partner)

    def ksum_x():
        ksum_all(kcore_ref, 0).wait_recv()
        kx_ref[x] = jnp.sum(kcore_ref[...], axis=0)
        loop(1, xs, lambda i: ksum_copy(kx_ref, x, 1, {"row_1": lax.rem(x + i, xs)}).start())

    def ksum_h():
        if xs > 1:
            ksum_all(kx_ref, 1).wait_recv()
        kh_ref[h] = jnp.sum(kx_ref[...], axis=0)
        loop(1, hs, lambda i: ksum_copy(kh_ref, h, 2, {"row_0": lax.rem(h + i, hs)}).start())

    def ksum_row():
        ksum_all(kh_ref, 2).wait_recv()
        return jnp.sum(kh_ref[...], axis=0)

    def ksum_of(sums, at):
        shape = (piece, sums.shape[1])
        here = lax.broadcasted_iota(jnp.int32, shape, 1) == lax.broadcasted_iota(jnp.int32, shape, 0) + at * piece
        return jnp.sum(jnp.where(here, sums, 0.0), axis=1, keepdims=True)

    def local_bias(dual, mult, signs, product_sum):
        steady = jnp.sum(signs * (dual - mult), axis=0, keepdims=True)
        return steady - (product_sum - jnp.sum(signs, axis=0, keepdims=True)) / penalty

    def update(q, dual, mult, signs, offset):
        w = dual - mult - (q - 1.0) / penalty
        hinge = jnp.maximum(0.0, 1.0 - q - signs * offset)
        gap = jnp.sum(dual * q - dual + box * hinge, axis=0, keepdims=True)
        x_value = w - signs * offset
        state = x_value + mult
        return state, clipped(state), state - clipped(state), gap

    def row_copies(s, i):
        j = flip(i)
        return (
            remote(row_send.at[s, j], row_recv.at[s, g], row_ss.at[s], row_rs.at[s], chip(i)),
            remote(rscale_send.at[s, lax.div(i, xs)], rscale_recv.at[s, g], rscale_ss.at[s], rscale_rs.at[s], chip(i)),
        )

    def row_all(s):
        rest = pl.ds(0, groups - 1)
        return (
            remote(row_send.at[s, rest], row_recv.at[s, rest], row_ss.at[s], row_rs.at[s], partner),
            remote(rscale_recv.at[s, rest], rscale_recv.at[s, rest], rscale_ss.at[s], rscale_rs.at[s], partner),
        )

    planes = sorted(range(hs), key=lambda d: -min(d, hs - d))

    def core_copy(s, plane):
        at = pl.ds(plane * xs, xs)
        return remote(
            part_ref.at[other, at], core_recv.at[s, at], core_ss.at[s, plane], core_rs.at[s, plane], partner
        )

    def core_sent(s):
        for plane in range(hs):
            core_copy(s, plane).wait_send()

    held = kernel_ref.shape[0]

    def transposed_part(which, plane):
        at = pl.multiple_of(which * half + plane * (xs * piece), 32)
        product = jnp.dot(
            turned_ref[pl.ds(at, xs * piece), :], weighted_ref[0:held, :], preferred_element_type=F32
        )
        part_ref[which, pl.ds(plane * xs, xs)] = product.reshape(xs, piece, settings)
        return jnp.sum(product, axis=0, keepdims=True)

    def transposed_send(s, before):
        for d in planes:
            plane = lax.rem(h + d, hs)
            before(d, plane)
            core_copy(s, plane).wait_recv()
            at = pl.ds(plane * xs, xs)
            both = part_ref[k, at] + core_recv[s, at]
            part_ref[k, at] = both
            row_send[s, at], rscale_send[s, plane] = coded(both)

            def send(i):
                for copy in row_copies(s, plane * xs + lax.rem(x + i, xs)):
                    copy.start()

            spread(xs, send)
            if d:
                send(0)

    def transposed_sum(s):
        row_recv[s, g] = jnp.zeros(row_recv.shape[2:], I16)
        rscale_recv[s, g] = jnp.zeros(rscale_recv.shape[2:], F32)
        for copy in row_all(s):
            copy.wait_recv()
        return part_ref[k, spot] + decoded_sum(row_recv[s], rscale_recv[s])


    load_k.wait()
    turned_ref[...] = jnp.transpose(kernel_ref[...])
    product_sum = zero
    for which in (other, k):
        for plane in range(hs):
            product_sum = product_sum + transposed_part(which, plane)
    ones = jnp.ones((8, kernel_ref.shape[0]), BF16)
    kcore_ref[k] = jnp.dot(ones, kernel_ref[...], preferred_element_type=F32)[0:1]
    pl.semaphore_wait(barrier, far_n - 1 + near_n - 1 + crossed)
    sum_start(0, local_bias(dual, mult, signs_row, product_sum), zero)
    for d in planes:
        core_copy(0, lax.rem(h + d, hs)).start()
    first_start()
    ksum_copy(kcore_ref, k, 0, partner).start()
    transposed_send(0, lambda d, plane: None)
    ksum_x()
    sum_middle(0)
    ksum_h()
    q_sum = transposed_sum(0)
    core_sent(0)
    dual, signs_col = first_arrived()
    mult = jnp.zeros_like(dual)
    offset = sum_end(0)[0:1] / total
    state, dual, mult, gap = update(signs_col * q_sum, dual, mult, signs_col, offset)

    gat_ref[mine] = (signs_col * dual).astype(BF16)

    def gat_copy(slot, send, recv, device):
        return remote(gat_ref.at[slot], gat_ref.at[slot], send, gat_rs.at[recv], device)

    spread(groups, lambda i: gat_copy(mine, gat_ss.at[0], spot, chip(lax.rem(g + i, groups))).start())
    gat_copy(mine, fwd_ss.at[0], groups, partner).start()
    ksum_send[...] = ksum_row()
    ksum = ksum_of(ksum_send[...], mine)
    weighted = gat_ref[mine].astype(F32)
    sum_start(1, local_bias(dual, mult, signs_col, jnp.sum(ksum * weighted, axis=0, keepdims=True)), gap)
    def forward(i):
        at = flip(lax.rem(g + i, groups))
        gat_copy(k * groups + at, fwd_ss.at[0], at, partner).wait_recv()
        gat_copy(k * groups + at, fwd_ss.at[0], groups, partner).start()

    loop(1, groups, forward)
    sum_middle(1)
    theirs = gat_ref.at[pl.ds(other * groups, groups)]
    remote(theirs, theirs, fwd_ss.at[0], gat_rs.at[groups], partner).wait_recv()
    move_state(0, state, to_row)
    move_ksum = remote(ksum_send, ksum_recv, kmove_sem.at[0], kmove_sem.at[1], to_row)
    move_ksum.start()
    weighted_ref[...] = gat_ref[...].astype(F32).reshape(rows * piece, -1).astype(BF16)
    per = 2 * ls
    quads = cols // per

    def col_start(i):
        remote(col_send.at[i], col_recv.at[c], col_ss.at[0], col_rs.at[0], column(i)).start()
        remote(
            cscale_send.at[lax.div(i, per)], cscale_recv.at[c], cscale_ss.at[0], cscale_rs.at[0], column(i)
        ).start()

    for d in sorted(range(quads), key=lambda d: -min(d, quads - d)):
        quad = lax.rem(lax.div(c, per) + d, quads)
        at = pl.ds(quad * per, per)
        product = jnp.dot(
            kernel_ref[pl.ds(pl.multiple_of(quad * (per * piece), 32), per * piece), :], weighted_ref[...],
            preferred_element_type=F32,
        ).reshape(per, piece, settings)
        part_ref[0, at] = product
        col_send[at], cscale_send[quad] = coded(product)
        if d:
            loop(0, per, lambda i: col_start(quad * per + i))
        else:
            loop(1, per, lambda i: col_start(quad * per + lax.rem(lax.rem(c, per) + i, per)))

    rest = pl.ds(0, cols - 1)
    col_all = (
        remote(col_send.at[rest], col_recv.at[rest], col_ss.at[0], col_rs.at[0], partner),
        remote(cscale_recv.at[rest], cscale_recv.at[rest], cscale_ss.at[0], cscale_rs.at[0], partner),
    )

    col_recv[c] = jnp.zeros(col_recv.shape[1:], I16)
    cscale_recv[c] = jnp.zeros(cscale_recv.shape[1:], F32)
    for copy in col_all:
        copy.wait_recv()
    q_sum = part_ref[0, c] + decoded_sum(col_recv[...], cscale_recv[...])
    dual, mult = arrived_state(0)
    sums = sum_end(1)
    gaps_out[0:1, :] = sums[1:2] / total
    offset = sums[0:1] / total
    state, dual, mult, gap = update(signs_row * q_sum, dual, mult, signs_row, offset)

    pcol_ref[c] = (signs_row * dual).astype(BF16)

    def pcol_copy(i):
        return remote(pcol_ref.at[c], pcol_ref.at[c], pcol_ss.at[0], pcol_rs.at[0], column(i))

    pcol_all = remote(pcol_ref.at[rest], pcol_ref.at[rest], pcol_ss.at[0], pcol_rs.at[0], partner)
    spread(cols, lambda i: pcol_copy(lax.rem(c + i, cols)).start())
    move_ksum.wait_recv()
    weighted = pcol_ref[c].astype(F32)
    ksum = ksum_of(ksum_recv[...], lax.rem(block, rows))
    sum_start(2, local_bias(dual, mult, signs_row, jnp.sum(ksum * weighted, axis=0, keepdims=True)), gap)
    pcol_all.wait_recv()
    move_state(1, state, to_column)
    weighted_ref[0:held, :] = pcol_ref[...].astype(F32).reshape(held, -1).astype(BF16)
    for d in planes:
        plane = lax.rem(h + d, hs)
        transposed_part(other, plane)
        core_copy(1, plane).start()
    sum_middle(2)
    transposed_send(1, lambda d, plane: transposed_part(k, plane))
    q_sum = transposed_sum(1)
    dual, mult = arrived_state(1)
    sums = sum_end(2)
    gaps_out[1:2, :] = sums[1:2] / total
    offset = sums[0:1] / total
    state, dual, mult, gap = update(signs_col * q_sum, dual, mult, signs_col, offset)

    sum_start(3, zero, gap)
    move_state(2, state, to_row)
    offset_out[...] = offset
    for t in range(3):
        near_all(t).wait_send()
        far_all(t).wait_send()
    state_copy(0, to_row).wait_send()
    state_copy(1, to_row).wait_send()
    core_sent(1)
    for copy in row_all(0) + row_all(1) + col_all:
        copy.wait_send()
    first_sent()
    rest = pl.ds(0, groups - 1)
    remote(gat_ref.at[rest], gat_ref.at[rest], gat_ss.at[0], gat_rs.at[0], partner).wait_send()
    rest = pl.ds(0, groups)
    remote(gat_ref.at[rest], gat_ref.at[rest], fwd_ss.at[0], gat_rs.at[0], partner).wait_send()
    pcol_all.wait_send()
    move_ksum.wait_send()
    ksum_all(kcore_ref, 0).wait_send()
    if xs > 1:
        ksum_all(kx_ref, 1).wait_send()
    ksum_all(kh_ref, 2).wait_send()
    sum_middle(3)
    state_copy(2, to_row).wait_send()
    dual_out[...], mult_out[...] = arrived_state(2)
    gaps_out[2:3, :] = sum_end(3)[1:2] / total
    near_all(3).wait_send()
    far_all(3).wait_send()


def hand_over(*refs):
    half = len(refs) // 2
    for source, target in zip(refs[:half], refs[half:]):
        target[...] = source[...]


def body(dims, kernel, labels, start_dual, penalty, box):
    hs, xs, ks, ys, ls = dims
    groups, rows, cols = hs * xs, hs * xs * ks, ys * ls
    height, width = kernel.shape
    settings = box.shape[0]
    piece = height // cols
    total = height * rows
    near_n, far_n = ys * ks, hs * xs * ls
    wide = 128 if height % 128 == 0 else height
    dma = pltpu.SemaphoreType.DMA
    vmem = pltpu.VMEM
    scratch = [
        vmem((height, width), BF16), vmem((width, height), BF16), vmem((width, settings), BF16), vmem((height // wide, wide), jnp.int32), vmem((height, settings), F32),
        vmem((1, settings), F32), vmem((1, settings), F32), vmem((height, settings), F32),
        vmem((ks, groups, piece, settings), F32), dma((5,)),
        vmem((piece, settings), F32), vmem((height // wide, wide), jnp.int32), vmem((height, settings), F32), dma((1 + groups // ls,)), dma((2,)),
        vmem((3, piece, settings), F32), vmem((3, piece, settings), F32), dma((3,)), dma((3,)),
        vmem((2, groups, piece, settings), F32), dma((2, hs)), dma((2, hs)),
        vmem((2, groups, piece, settings), I16), vmem((2, groups, piece, settings), I16), dma((2,)), dma((2,)),
        vmem((2, hs, 1, settings), F32), vmem((2, groups, 1, settings), F32), dma((2,)), dma((2,)),
        vmem((rows, piece, settings), BF16), dma((1,)), dma((groups + 1,)), dma((1,)),
        vmem((cols, piece, settings), I16), vmem((cols, piece, settings), I16), dma((1,)), dma((1,)),
        vmem((cols // (2 * ls), 1, settings), F32), vmem((cols, 1, settings), F32), dma((1,)), dma((1,)),
        vmem((cols, piece, settings), BF16), dma((1,)), dma((1,)),
        vmem((4, near_n, 2, settings), F32), dma((4,)), dma((4,)),
        vmem((4, far_n, 2, settings), F32), dma((4,)), dma((4,)),
        vmem((ks, 1, width), F32), vmem((xs, 1, width), F32), vmem((hs, 1, width), F32), dma((3,)), dma((3,)),
        vmem((1, width), F32), vmem((1, width), F32), dma((2,)),
    ]
    in_vmem = pl.BlockSpec(memory_space=vmem)
    in_hbm = pl.BlockSpec(memory_space=pltpu.HBM)
    outs_shape = tuple(
        jax.ShapeDtypeStruct(shape, F32)
        for shape in ((piece, settings), (piece, settings), (ITERS, settings), (1, settings))
    )
    kept = tuple(vmem(shape.shape, F32) for shape in outs_shape)
    outs = pl.pallas_call(
        functools.partial(admm, dims, total),
        out_shape=kept,
        in_specs=[in_hbm] * 5,
        out_specs=(in_vmem,) * 4,
        scratch_shapes=scratch,
        compiler_params=pltpu.CompilerParams(collective_id=0, has_side_effects=True),
        name="admm",
    )(kernel, labels.reshape(height // wide, wide), start_dual, penalty[None, :], box[None, :])
    outs = [pltpu.with_memory_space_constraint(out, vmem) for out in outs]
    dual, mult, gaps, offset = pl.pallas_call(
        hand_over, out_shape=outs_shape, in_specs=[in_vmem] * 4, out_specs=(in_vmem,) * 4, name="hand_over"
    )(*outs)
    return dual, mult, gaps, offset[0]


def build(torus):
    dims = torus.devices.shape
    in_specs = (P(ROW, COL), P(ROW), P(ROW, None), P(), P())
    out_specs = (P(ROW_COL, None), P(ROW_COL, None), P(), P())
    return jax.shard_map(
        functools.partial(body, dims), mesh=torus, in_specs=in_specs, out_specs=out_specs, check_vma=False
    )


def solution(mesh):
    return build(Mesh(mesh.devices.reshape(4, 4, 2, 8, 2), ROW_COL))
```

```python
import functools

import jax
import jax.numpy as jnp
from jax import lax
from jax.experimental import pallas as pl
from jax.experimental.pallas import tpu as pltpu
from jax.sharding import Mesh
from jax.sharding import PartitionSpec as P

ITERS = 3
ROW = ("row_0", "row_1", "row_2")
COL = ("col_0", "col_1")
ROW_COL = ROW + COL
MESH = pl.DeviceIdType.MESH
F32 = jnp.float32
BF16 = jnp.bfloat16
I16 = jnp.int16
LEVELS = 32767.0


def loop(low, high, step):
    def one(i, carry):
        step(i)
        return carry

    lax.fori_loop(low, high, one, jnp.int32(0))


def spread(count, step):
    def one(j):
        step(count // 2 + lax.div(j + 1, 2) * (2 * lax.rem(j, 2) - 1))

    loop(0, count - 1, one)


def flip(i):
    return i + 1 - 2 * lax.rem(i, 2)


def coded(values):
    most = jnp.maximum(jnp.max(jnp.max(jnp.abs(values), axis=0), axis=0, keepdims=True), 1e-30)
    return jnp.round(values * (LEVELS / most)).astype(jnp.int32).astype(I16), most / LEVELS


def decoded_sum(codes, scales):
    return jnp.sum(codes.astype(jnp.int32).astype(F32) * scales, axis=0)


def write_signs(labels_ref, signs_ref):
    wide = labels_ref.shape[1]
    for i in range(labels_ref.shape[0]):
        line = labels_ref[i : i + 1, :].astype(F32)
        if wide == 128:
            block_signs = jnp.transpose(jnp.broadcast_to(line, (128, 128)))
        else:
            block_signs = jnp.broadcast_to(jnp.transpose(line), (wide, 128))
        signs_ref[i * wide : (i + 1) * wide, :] = block_signs


def remote(src, dst, send, recv, device):
    return pltpu.make_async_remote_copy(
        src_ref=src, dst_ref=dst, send_sem=send, recv_sem=recv, device_id=device, device_id_type=MESH
    )


def admm(
    dims, total,
    kernel_hbm, labels_hbm, start_hbm, penalty_hbm, box_hbm,
    dual_out, mult_out, gaps_out, offset_out,
    kernel_ref, turned_ref, weighted_ref, labels_ref, start_ref, penalty_ref, box_ref, signs_ref, part_ref,
    load_sem,
    first_ref, first_labels_ref, first_signs_ref, first_ss, first_rs,
    state_send, state_recv, state_ss, state_rs,
    core_recv, core_ss, core_rs,
    row_send, row_recv, row_ss, row_rs, rscale_send, rscale_recv, rscale_ss, rscale_rs,
    gat_ref, gat_ss, gat_rs, fwd_ss,
    col_send, col_recv, col_ss, col_rs, cscale_send, cscale_recv, cscale_ss, cscale_rs,
    pcol_ref, pcol_ss, pcol_rs,
    near_ref, near_ss, near_rs,
    far_ref, far_ss, far_rs,
    kcore_ref, kx_ref, kh_ref, ksum_ss, ksum_rs, ksum_send, ksum_recv, kmove_sem,
):
    hs, xs, ks, ys, ls = dims
    groups, rows, cols = hs * xs, hs * xs * ks, ys * ls
    h, x, k = (lax.axis_index(a) for a in ROW)
    y, l = (lax.axis_index(a) for a in COL)
    g = h * xs + x
    r = g * ks + k
    c = y * ls + l
    piece, settings = state_send.shape[1:]
    half = groups * piece
    near_n, far_n = ys * ks, hs * xs * ls
    near_me = y * ks + k
    far_me = g * ls + l
    other = 1 - k

    def chip(to):
        return {"row_0": lax.div(to, xs), "row_1": lax.rem(to, xs)}

    def column(to):
        return {"col_0": lax.div(to, ls), "col_1": lax.rem(to, ls)}

    def whole(row, col):
        return {
            "row_0": lax.div(row, xs * ks), "row_1": lax.rem(lax.div(row, ks), xs), "row_2": lax.rem(row, ks),
            "col_0": lax.div(col, ls), "col_1": lax.rem(col, ls),
        }

    def near(to):
        return {"row_2": lax.rem(to, ks), "col_0": lax.div(to, ks)}

    def far(to):
        on = lax.div(to, ls)
        return {"row_0": lax.div(on, xs), "row_1": lax.rem(on, xs), "col_1": lax.rem(to, ls)}

    partner = {"row_2": other}
    spot = flip(g)
    mine = k * groups + spot
    block = r * cols + c
    to_piece = lax.rem(block, rows)
    to_column = whole(
        flip(lax.rem(to_piece, groups)) * ks + lax.div(to_piece, groups), lax.div(block, rows)
    )
    owned = c * rows + mine
    to_row = whole(lax.div(owned, cols), lax.rem(owned, cols))

    load_k = pltpu.make_async_copy(kernel_hbm, kernel_ref, load_sem.at[0])
    load_s = pltpu.make_async_copy(start_hbm, start_ref, load_sem.at[1])
    load_l = pltpu.make_async_copy(labels_hbm, labels_ref, load_sem.at[2])
    load_p = pltpu.make_async_copy(penalty_hbm, penalty_ref, load_sem.at[3])
    load_b = pltpu.make_async_copy(box_hbm, box_ref, load_sem.at[4])
    load_l.start()
    load_b.start()
    load_s.start()
    load_p.start()
    load_k.start()

    barrier = pltpu.get_barrier_semaphore()

    def greet(device):
        pl.semaphore_signal(barrier, inc=1, device_id=device, device_id_type=MESH)

    spread(far_n, lambda i: greet(far(lax.rem(far_me + i, far_n))))
    loop(1, near_n, lambda i: greet(near(lax.rem(near_me + i, near_n))))
    load_l.wait()
    write_signs(labels_ref, signs_ref)
    load_b.wait()
    load_s.wait()
    load_p.wait()
    penalty = penalty_ref[...]
    box = box_ref[...]
    def clipped(values):
        return jnp.minimum(jnp.maximum(values, 0.0), box)

    weighted_ref[0 : start_ref.shape[0], :] = (signs_ref[...] * clipped(start_ref[...])).astype(BF16)
    own_rows = pl.ds(pl.multiple_of(c * piece, 8), piece)
    signs_row = signs_ref[own_rows, :]
    dual = clipped(start_ref[own_rows, :])
    mult = jnp.zeros_like(dual)
    zero = jnp.zeros((1, settings), F32)

    from_here = lax.div(g, ls) == y
    to_side = lax.rem(g, ls)

    def first_copies(j, device):
        rows_j = pl.ds(pl.multiple_of(j * piece, 8), piece)
        return (
            remote(start_ref.at[rows_j], first_ref, first_ss.at[0], first_rs.at[0], device),
            remote(labels_ref, first_labels_ref, first_ss.at[1 + lax.div(j, ls)], first_rs.at[1], device),
        )

    def first_start():
        def one(i):
            j = i * ls + l
            for copy in first_copies(j, chip(flip(j)) | {"col_1": to_side}):
                copy.start()

        @pl.when(from_here)
        def _():
            loop(0, groups // ls, one)

    def first_sent():
        @pl.when(from_here)
        def _():
            sent = start_ref.at[pl.ds(0, groups // ls * piece)]
            remote(sent, sent, first_ss.at[0], first_rs.at[0], partner).wait_send()
            loop(0, groups // ls, lambda i: first_copies(i * ls + l, partner)[1].wait_send())

    def first_arrived():
        for copy in first_copies(0, partner):
            copy.wait_recv()
        write_signs(first_labels_ref, first_signs_ref)
        return clipped(first_ref[...]), first_signs_ref[pl.ds(pl.multiple_of(spot * piece, 8), piece), :]

    def state_copy(t, device):
        return remote(state_send.at[t], state_recv.at[t], state_ss.at[t], state_rs.at[t], device)

    def move_state(t, state, device):
        state_send[t] = state
        state_copy(t, device).start()

    def arrived_state(t):
        state_copy(t, to_row).wait_recv()
        state = state_recv[t]
        return clipped(state), state - clipped(state)

    def near_copy(t, i):
        return remote(near_ref.at[t, near_me], near_ref.at[t, near_me], near_ss.at[t], near_rs.at[t], near(i))

    def near_all(t):
        rest = near_ref.at[t, pl.ds(0, near_n - 1)]
        return remote(rest, rest, near_ss.at[t], near_rs.at[t], partner)

    def far_copy(t, i):
        return remote(far_ref.at[t, far_me], far_ref.at[t, far_me], far_ss.at[t], far_rs.at[t], far(i))

    def far_all(t):
        rest = far_ref.at[t, pl.ds(0, far_n - 1)]
        return remote(rest, rest, far_ss.at[t], far_rs.at[t], partner)

    def sum_start(t, top, bottom):
        near_ref[t, near_me, 0:1, :] = top
        near_ref[t, near_me, 1:2, :] = bottom
        spread(near_n, lambda i: near_copy(t, lax.rem(near_me + i, near_n)).start())

    def sum_middle(t):
        near_all(t).wait_recv()
        far_ref[t, far_me] = jnp.sum(near_ref[t], axis=0)
        spread(far_n, lambda i: far_copy(t, lax.rem(far_me + i, far_n)).start())

    def sum_end(t):
        far_all(t).wait_recv()
        return jnp.sum(far_ref[t], axis=0)

    def ksum_copy(ref, slot, stage, device):
        return remote(ref.at[slot], ref.at[slot], ksum_ss.at[stage], ksum_rs.at[stage], device)

    def ksum_all(ref, stage):
        rest = ref.at[pl.ds(0, ref.shape[0] - 1)]
        return remote(rest, rest, ksum_ss.at[stage], ksum_rs.at[stage], partner)

    def ksum_x():
        ksum_all(kcore_ref, 0).wait_recv()
        kx_ref[x] = jnp.sum(kcore_ref[...], axis=0)
        loop(1, xs, lambda i: ksum_copy(kx_ref, x, 1, {"row_1": lax.rem(x + i, xs)}).start())

    def ksum_h():
        if xs > 1:
            ksum_all(kx_ref, 1).wait_recv()
        kh_ref[h] = jnp.sum(kx_ref[...], axis=0)
        loop(1, hs, lambda i: ksum_copy(kh_ref, h, 2, {"row_0": lax.rem(h + i, hs)}).start())

    def ksum_row():
        ksum_all(kh_ref, 2).wait_recv()
        return jnp.sum(kh_ref[...], axis=0)

    def ksum_of(sums, at):
        shape = (piece, sums.shape[1])
        here = lax.broadcasted_iota(jnp.int32, shape, 1) == lax.broadcasted_iota(jnp.int32, shape, 0) + at * piece
        return jnp.sum(jnp.where(here, sums, 0.0), axis=1, keepdims=True)

    def local_bias(dual, mult, signs, product_sum):
        steady = jnp.sum(signs * (dual - mult), axis=0, keepdims=True)
        return steady - (product_sum - jnp.sum(signs, axis=0, keepdims=True)) / penalty

    def update(q, dual, mult, signs, offset):
        w = dual - mult - (q - 1.0) / penalty
        hinge = jnp.maximum(0.0, 1.0 - q - signs * offset)
        gap = jnp.sum(dual * q - dual + box * hinge, axis=0, keepdims=True)
        x_value = w - signs * offset
        state = x_value + mult
        return state, clipped(state), state - clipped(state), gap

    def row_copies(s, i):
        j = flip(i)
        return (
            remote(row_send.at[s, j], row_recv.at[s, g], row_ss.at[s], row_rs.at[s], chip(i)),
            remote(rscale_send.at[s, lax.div(i, xs)], rscale_recv.at[s, g], rscale_ss.at[s], rscale_rs.at[s], chip(i)),
        )

    def row_all(s):
        rest = pl.ds(0, groups - 1)
        return (
            remote(row_send.at[s, rest], row_recv.at[s, rest], row_ss.at[s], row_rs.at[s], partner),
            remote(rscale_recv.at[s, rest], rscale_recv.at[s, rest], rscale_ss.at[s], rscale_rs.at[s], partner),
        )

    planes = sorted(range(hs), key=lambda d: -min(d, hs - d))

    def core_copy(s, plane):
        at = pl.ds(plane * xs, xs)
        return remote(
            part_ref.at[other, at], core_recv.at[s, at], core_ss.at[s, plane], core_rs.at[s, plane], partner
        )

    def core_sent(s):
        for plane in range(hs):
            core_copy(s, plane).wait_send()

    held = kernel_ref.shape[0]

    def transposed_part(which, plane):
        at = pl.multiple_of(which * half + plane * (xs * piece), 32)
        product = jnp.dot(
            turned_ref[pl.ds(at, xs * piece), :], weighted_ref[0:held, :], preferred_element_type=F32
        )
        part_ref[which, pl.ds(plane * xs, xs)] = product.reshape(xs, piece, settings)
        return jnp.sum(product, axis=0, keepdims=True)

    def transposed_send(s, before):
        for d in planes:
            plane = lax.rem(h + d, hs)
            before(d, plane)
            core_copy(s, plane).wait_recv()
            at = pl.ds(plane * xs, xs)
            both = part_ref[k, at] + core_recv[s, at]
            part_ref[k, at] = both
            row_send[s, at], rscale_send[s, plane] = coded(both)

            def send(i):
                for copy in row_copies(s, plane * xs + lax.rem(x + i, xs)):
                    copy.start()

            spread(xs, send)
            if d:
                send(0)

    def transposed_sum(s):
        row_recv[s, g] = jnp.zeros(row_recv.shape[2:], I16)
        rscale_recv[s, g] = jnp.zeros(rscale_recv.shape[2:], F32)
        for copy in row_all(s):
            copy.wait_recv()
        return part_ref[k, spot] + decoded_sum(row_recv[s], rscale_recv[s])


    load_k.wait()
    turned_ref[...] = jnp.transpose(kernel_ref[...])
    product_sum = zero
    for which in (other, k):
        for plane in range(hs):
            product_sum = product_sum + transposed_part(which, plane)
    ones = jnp.ones((8, kernel_ref.shape[0]), BF16)
    kcore_ref[k] = jnp.dot(ones, kernel_ref[...], preferred_element_type=F32)[0:1]
    pl.semaphore_wait(barrier, far_n - 1 + near_n - 1)
    sum_start(0, local_bias(dual, mult, signs_row, product_sum), zero)
    for d in planes:
        core_copy(0, lax.rem(h + d, hs)).start()
    first_start()
    ksum_copy(kcore_ref, k, 0, partner).start()
    transposed_send(0, lambda d, plane: None)
    ksum_x()
    sum_middle(0)
    ksum_h()
    q_sum = transposed_sum(0)
    core_sent(0)
    dual, signs_col = first_arrived()
    mult = jnp.zeros_like(dual)
    offset = sum_end(0)[0:1] / total
    state, dual, mult, gap = update(signs_col * q_sum, dual, mult, signs_col, offset)

    gat_ref[mine] = (signs_col * dual).astype(BF16)

    def gat_copy(slot, send, recv, device):
        return remote(gat_ref.at[slot], gat_ref.at[slot], send, gat_rs.at[recv], device)

    spread(groups, lambda i: gat_copy(mine, gat_ss.at[0], spot, chip(lax.rem(g + i, groups))).start())
    gat_copy(mine, fwd_ss.at[0], groups, partner).start()
    ksum_send[...] = ksum_row()
    ksum = ksum_of(ksum_send[...], mine)
    weighted = gat_ref[mine].astype(F32)
    sum_start(1, local_bias(dual, mult, signs_col, jnp.sum(ksum * weighted, axis=0, keepdims=True)), gap)
    def forward(i):
        at = flip(lax.rem(g + i, groups))
        gat_copy(k * groups + at, fwd_ss.at[0], at, partner).wait_recv()
        gat_copy(k * groups + at, fwd_ss.at[0], groups, partner).start()

    loop(1, groups, forward)
    sum_middle(1)
    theirs = gat_ref.at[pl.ds(other * groups, groups)]
    remote(theirs, theirs, fwd_ss.at[0], gat_rs.at[groups], partner).wait_recv()
    move_state(0, state, to_row)
    move_ksum = remote(ksum_send, ksum_recv, kmove_sem.at[0], kmove_sem.at[1], to_row)
    move_ksum.start()
    weighted_ref[...] = gat_ref[...].astype(F32).reshape(rows * piece, -1).astype(BF16)
    per = 2 * ls
    quads = cols // per

    def col_start(i):
        remote(col_send.at[i], col_recv.at[c], col_ss.at[0], col_rs.at[0], column(i)).start()
        remote(
            cscale_send.at[lax.div(i, per)], cscale_recv.at[c], cscale_ss.at[0], cscale_rs.at[0], column(i)
        ).start()

    for d in sorted(range(quads), key=lambda d: -min(d, quads - d)):
        quad = lax.rem(lax.div(c, per) + d, quads)
        at = pl.ds(quad * per, per)
        product = jnp.dot(
            kernel_ref[pl.ds(pl.multiple_of(quad * (per * piece), 32), per * piece), :], weighted_ref[...],
            preferred_element_type=F32,
        ).reshape(per, piece, settings)
        part_ref[0, at] = product
        col_send[at], cscale_send[quad] = coded(product)
        if d:
            loop(0, per, lambda i: col_start(quad * per + i))
        else:
            loop(1, per, lambda i: col_start(quad * per + lax.rem(lax.rem(c, per) + i, per)))

    rest = pl.ds(0, cols - 1)
    col_all = (
        remote(col_send.at[rest], col_recv.at[rest], col_ss.at[0], col_rs.at[0], partner),
        remote(cscale_recv.at[rest], cscale_recv.at[rest], cscale_ss.at[0], cscale_rs.at[0], partner),
    )

    col_recv[c] = jnp.zeros(col_recv.shape[1:], I16)
    cscale_recv[c] = jnp.zeros(cscale_recv.shape[1:], F32)
    for copy in col_all:
        copy.wait_recv()
    q_sum = part_ref[0, c] + decoded_sum(col_recv[...], cscale_recv[...])
    dual, mult = arrived_state(0)
    sums = sum_end(1)
    gaps_out[0:1, :] = sums[1:2] / total
    offset = sums[0:1] / total
    state, dual, mult, gap = update(signs_row * q_sum, dual, mult, signs_row, offset)

    pcol_ref[c] = (signs_row * dual).astype(BF16)

    def pcol_copy(i):
        return remote(pcol_ref.at[c], pcol_ref.at[c], pcol_ss.at[0], pcol_rs.at[0], column(i))

    pcol_all = remote(pcol_ref.at[rest], pcol_ref.at[rest], pcol_ss.at[0], pcol_rs.at[0], partner)
    spread(cols, lambda i: pcol_copy(lax.rem(c + i, cols)).start())
    move_ksum.wait_recv()
    weighted = pcol_ref[c].astype(F32)
    ksum = ksum_of(ksum_recv[...], lax.rem(block, rows))
    sum_start(2, local_bias(dual, mult, signs_row, jnp.sum(ksum * weighted, axis=0, keepdims=True)), gap)
    pcol_all.wait_recv()
    move_state(1, state, to_column)
    weighted_ref[0:held, :] = pcol_ref[...].astype(F32).reshape(held, -1).astype(BF16)
    for d in planes:
        plane = lax.rem(h + d, hs)
        transposed_part(other, plane)
        core_copy(1, plane).start()
    sum_middle(2)
    transposed_send(1, lambda d, plane: transposed_part(k, plane))
    q_sum = transposed_sum(1)
    dual, mult = arrived_state(1)
    sums = sum_end(2)
    gaps_out[1:2, :] = sums[1:2] / total
    offset = sums[0:1] / total
    state, dual, mult, gap = update(signs_col * q_sum, dual, mult, signs_col, offset)

    sum_start(3, zero, gap)
    move_state(2, state, to_row)
    offset_out[...] = offset
    for t in range(3):
        near_all(t).wait_send()
        far_all(t).wait_send()
    state_copy(0, to_row).wait_send()
    state_copy(1, to_row).wait_send()
    core_sent(1)
    for copy in row_all(0) + row_all(1) + col_all:
        copy.wait_send()
    first_sent()
    rest = pl.ds(0, groups - 1)
    remote(gat_ref.at[rest], gat_ref.at[rest], gat_ss.at[0], gat_rs.at[0], partner).wait_send()
    rest = pl.ds(0, groups)
    remote(gat_ref.at[rest], gat_ref.at[rest], fwd_ss.at[0], gat_rs.at[0], partner).wait_send()
    pcol_all.wait_send()
    move_ksum.wait_send()
    ksum_all(kcore_ref, 0).wait_send()
    if xs > 1:
        ksum_all(kx_ref, 1).wait_send()
    ksum_all(kh_ref, 2).wait_send()
    sum_middle(3)
    state_copy(2, to_row).wait_send()
    dual_out[...], mult_out[...] = arrived_state(2)
    gaps_out[2:3, :] = sum_end(3)[1:2] / total
    near_all(3).wait_send()
    far_all(3).wait_send()


def hand_over(*refs):
    half = len(refs) // 2
    for source, target in zip(refs[:half], refs[half:]):
        target[...] = source[...]


def body(dims, kernel, labels, start_dual, penalty, box):
    hs, xs, ks, ys, ls = dims
    groups, rows, cols = hs * xs, hs * xs * ks, ys * ls
    height, width = kernel.shape
    settings = box.shape[0]
    piece = height // cols
    total = height * rows
    near_n, far_n = ys * ks, hs * xs * ls
    wide = 128 if height % 128 == 0 else height
    dma = pltpu.SemaphoreType.DMA
    vmem = pltpu.VMEM
    scratch = [
        vmem((height, width), BF16), vmem((width, height), BF16), vmem((width, settings), BF16), vmem((height // wide, wide), jnp.int32), vmem((height, settings), F32),
        vmem((1, settings), F32), vmem((1, settings), F32), vmem((height, settings), F32),
        vmem((ks, groups, piece, settings), F32), dma((5,)),
        vmem((piece, settings), F32), vmem((height // wide, wide), jnp.int32), vmem((height, settings), F32), dma((1 + groups // ls,)), dma((2,)),
        vmem((3, piece, settings), F32), vmem((3, piece, settings), F32), dma((3,)), dma((3,)),
        vmem((2, groups, piece, settings), F32), dma((2, hs)), dma((2, hs)),
        vmem((2, groups, piece, settings), I16), vmem((2, groups, piece, settings), I16), dma((2,)), dma((2,)),
        vmem((2, hs, 1, settings), F32), vmem((2, groups, 1, settings), F32), dma((2,)), dma((2,)),
        vmem((rows, piece, settings), BF16), dma((1,)), dma((groups + 1,)), dma((1,)),
        vmem((cols, piece, settings), I16), vmem((cols, piece, settings), I16), dma((1,)), dma((1,)),
        vmem((cols // (2 * ls), 1, settings), F32), vmem((cols, 1, settings), F32), dma((1,)), dma((1,)),
        vmem((cols, piece, settings), BF16), dma((1,)), dma((1,)),
        vmem((4, near_n, 2, settings), F32), dma((4,)), dma((4,)),
        vmem((4, far_n, 2, settings), F32), dma((4,)), dma((4,)),
        vmem((ks, 1, width), F32), vmem((xs, 1, width), F32), vmem((hs, 1, width), F32), dma((3,)), dma((3,)),
        vmem((1, width), F32), vmem((1, width), F32), dma((2,)),
    ]
    in_vmem = pl.BlockSpec(memory_space=vmem)
    in_hbm = pl.BlockSpec(memory_space=pltpu.HBM)
    outs_shape = tuple(
        jax.ShapeDtypeStruct(shape, F32)
        for shape in ((piece, settings), (piece, settings), (ITERS, settings), (1, settings))
    )
    kept = tuple(vmem(shape.shape, F32) for shape in outs_shape)
    outs = pl.pallas_call(
        functools.partial(admm, dims, total),
        out_shape=kept,
        in_specs=[in_hbm] * 5,
        out_specs=(in_vmem,) * 4,
        scratch_shapes=scratch,
        compiler_params=pltpu.CompilerParams(collective_id=0, has_side_effects=True),
        name="admm",
    )(kernel, labels.reshape(height // wide, wide), start_dual, penalty[None, :], box[None, :])
    outs = [pltpu.with_memory_space_constraint(out, vmem) for out in outs]
    dual, mult, gaps, offset = pl.pallas_call(
        hand_over, out_shape=outs_shape, in_specs=[in_vmem] * 4, out_specs=(in_vmem,) * 4, name="hand_over"
    )(*outs)
    return dual, mult, gaps, offset[0]


def build(torus):
    dims = torus.devices.shape
    in_specs = (P(ROW, COL), P(ROW), P(ROW, None), P(), P())
    out_specs = (P(ROW_COL, None), P(ROW_COL, None), P(), P())
    return jax.shard_map(
        functools.partial(body, dims), mesh=torus, in_specs=in_specs, out_specs=out_specs, check_vma=False
    )


def solution(mesh):
    return build(Mesh(mesh.devices.reshape(4, 4, 2, 8, 2), ROW_COL))
```
